32 devices in a mesh: dp: 8 (over z, y), mp: 4 (over x, core).
Axes of the slice: x: 2, y: 2, z: 4, core: 2. Of those that a mesh axis runs over, the one named last changes fastest.
Arguments:
- inputs: bfloat16 [32, 1024, 768], P(('dp', 'mp')), may hold values from -6 to 6
- lengths: int32 [32], P('dp'), may hold values from 102 to 1024, as said below
- w_query: bfloat16 [768, 768], P(None, 'mp'), may hold values from -0.21875 to 0.21875
- b_query: bfloat16 [768], P('mp'), may hold values from -3 to 3
- w_key: bfloat16 [768, 768], P(None, 'mp'), may hold values from -0.21875 to 0.21875
- w_value: bfloat16 [768, 768], P(None, 'mp'), may hold values from -0.21875 to 0.21875
- b_value: bfloat16 [768], P('mp'), may hold values from -3 to 3
- w_out: bfloat16 [768, 768], P('mp'), may hold values from -6 to 6
- b_out: bfloat16 [768], replicated, may hold values from -3 to 3
- gain_one: bfloat16 [768], replicated, may hold values from 0.5 to 1.5
- shift_one: bfloat16 [768], replicated, may hold values from -2 to 2
- w_up: bfloat16 [768, 3072], P(None, 'mp'), may hold values from -0.21875 to 0.21875
- b_up: bfloat16 [3072], P('mp'), may hold values from -3 to 3
- w_down: bfloat16 [3072, 768], P('mp'), may hold values from -0.109375 to 0.109375
- b_down: bfloat16 [768], replicated, may hold values from -3 to 3
- gain_two: bfloat16 [768], replicated, may hold values from 0.5 to 1.5
- shift_two: bfloat16 [768], replicated, may hold values from -2 to 2
- cotangent: bfloat16 [32, 1024, 768], P(('dp', 'mp')), may hold values from -6 to 6
Outputs:
- output: bfloat16 [32, 1024, 768], P(('dp', 'mp'))
- grad_inputs: bfloat16 [32, 1024, 768], P(('dp', 'mp'))
- grad_w_query: float32 [768, 768], P(None, 'mp')
- grad_b_query: float32 [768], P('mp')
- grad_w_key: float32 [768, 768], P(None, 'mp')
- grad_w_value: float32 [768, 768], P(None, 'mp')
- grad_b_value: float32 [768], P('mp')
- grad_w_out: float32 [768, 768], P('mp')
- grad_b_out: float32 [768], replicated
- grad_gain_one: float32 [768], replicated
- grad_shift_one: float32 [768], replicated
- grad_w_up: float32 [768, 3072], P(None, 'mp')
- grad_b_up: float32 [3072], P('mp')
- grad_w_down: float32 [3072, 768], P('mp')
- grad_b_down: float32 [768], replicated
- grad_gain_two: float32 [768], replicated
- grad_shift_two: float32 [768], replicated
The draws below stay inside these ranges and needn't reach their ends.
Inputs may be any that keep to these rules, and one draw needn't show every extreme that they name: `lengths`: valid frames of each clip; the frames after them are padding and no query attends to them; one clip has all 1024 frames valid.
All inputs are finite; a program needn't handle non-finite values.
Results may differ from the reference program's by a relative error of at most 0.02.
Values may be sent and summed in bfloat16 or wider, within the bound.
A program may use at most 192 MiB of HBM per device.

```python
import jax
import jax.numpy as jnp
from jax import lax

D = 768
HEADS = 12
FF = 3072
HD = 64
LEN = 1024
CLIPS = 32


def draw_lengths(key, part):
    low_end = max(LEN // 10, 2)
    drawn_len = jax.random.randint(key, (CLIPS,), low_end, LEN + 1)
    picked = jax.random.randint(jax.random.fold_in(key, 7), (), 0, CLIPS)
    return jnp.where(jnp.arange(CLIPS) == picked, LEN, drawn_len).astype(jnp.int32)


def shard_levels(rng, extent, pieces, smallest, largest):
    def one(dim, blocks):
        draws = jax.random.uniform(jax.random.fold_in(jax.random.fold_in(rng, 6), dim), (blocks,), jnp.float32, smallest / len(pieces), largest / len(pieces))
        return jnp.repeat(jnp.exp(draws), extent[dim] // blocks).reshape((-1,) + (1,) * (len(extent) - dim - 1))

    factor_of = one(*pieces[0])
    for cut in pieces[1:]:
        factor_of = factor_of * one(*cut)
    return factor_of


def gaussian(own_key, extent, scale, bound, split=(), kind=jnp.bfloat16):
    array = scale * jax.random.normal(own_key, extent, jnp.float32)
    if split:
        array = array * shard_levels(own_key, extent, split, -0.22, 0.18)
    return jnp.clip(array, -bound, bound).astype(kind)


def setup_inputs(seed: int = 0) -> dict:
    key_list = jax.random.split(jax.random.key(seed), 19)
    inputs = gaussian(key_list[0], (CLIPS, LEN, D), 1.0, 6.0, ((0, 32),))
    lengths = draw_lengths(jax.random.fold_in(key_list[18], 71), 0)
    w_query = gaussian(key_list[2], (D, D), D ** -0.5, 0.21875, ((1, 4),))
    b_query = gaussian(key_list[3], (D,), 0.5, 3.0, ((0, 4),))
    w_key = gaussian(key_list[4], (D, D), D ** -0.5, 0.21875, ((1, 4),))
    w_value = gaussian(key_list[5], (D, D), D ** -0.5, 0.21875, ((1, 4),))
    b_value = gaussian(key_list[6], (D,), 0.5, 3.0, ((0, 4),))
    w_out = gaussian(key_list[7], (D, D), (max(2 * D // LEN, 1)) ** -0.5, 6.0, ((0, 4),))
    b_out = gaussian(key_list[8], (D,), 0.5, 3.0)
    gain_one = jnp.clip(1.0 + 0.1 * jax.random.normal(key_list[9], (D,), jnp.float32), 0.5, 1.5).astype(jnp.bfloat16)
    shift_one = gaussian(key_list[10], (D,), 0.3, 2.0)
    w_up = gaussian(key_list[11], (D, FF), D ** -0.5, 0.21875, ((1, 4),))
    b_up = gaussian(key_list[12], (FF,), 0.5, 3.0, ((0, 4),))
    w_down = gaussian(key_list[13], (FF, D), FF ** -0.5, 0.109375, ((0, 4),))
    b_down = gaussian(key_list[14], (D,), 0.5, 3.0)
    gain_two = jnp.clip(1.0 + 0.1 * jax.random.normal(key_list[15], (D,), jnp.float32), 0.5, 1.5).astype(jnp.bfloat16)
    shift_two = gaussian(key_list[16], (D,), 0.3, 2.0)
    cotangent = gaussian(key_list[17], (CLIPS, LEN, D), 1.0, 6.0, ((0, 32),))
    return dict(inputs=inputs, lengths=lengths, w_query=w_query, b_query=b_query, w_key=w_key, w_value=w_value, b_value=b_value, w_out=w_out, b_out=b_out, gain_one=gain_one, shift_one=shift_one, w_up=w_up, b_up=b_up, w_down=w_down, b_down=b_down, gain_two=gain_two, shift_two=shift_two, cotangent=cotangent)


@jax.custom_vjp
def low(v):
    return lax.optimization_barrier(v.astype(jnp.bfloat16)).astype(jnp.float32)

@jax.custom_vjp
def low_back(v):
    return v

def low_keep(v):
    return (low(v), None)

def low_pass(kept, grad):
    return (grad,)

def back_keep(v):
    return (v, None)

def back_low(kept, grad):
    return (low(grad),)
low.defvjp(low_keep, low_pass)
low_back.defvjp(back_keep, back_low)
epsilon = 1e-05

def product(left, right):
    return jnp.dot(left, right, precision=lax.Precision.HIGHEST)

def layer_norm(summed, gain_vec, shift_vec):
    centered = summed - lax.optimization_barrier(jnp.mean(summed, -1, keepdims=True))
    inv_root = lax.rsqrt(lax.optimization_barrier(jnp.mean(centered * centered, -1, keepdims=True)) + epsilon)
    return centered * inv_root * gain_vec + shift_vec

def clip_layer(frames_in, length, params):
    w_query, b_query, w_key, w_value, b_value, w_out, b_out, gain_one, shift_one, w_up, b_up, w_down, b_down, gain_two, shift_two = params
    scaling = HD ** (-0.5)
    sent_rows = low(frames_in)
    queries = low(low_back(product(sent_rows, w_query) + b_query))
    key_rows = low(low_back(product(sent_rows, w_key)))
    values = low(low_back(product(sent_rows, w_value) + b_value))
    head_shape = (LEN, HEADS, HD)
    scores = jnp.einsum('qhd,khd->hqk', queries.reshape(head_shape), key_rows.reshape(head_shape), precision=lax.Precision.HIGHEST)
    scores = low_back(scores * scaling)
    valid_key = jnp.arange(LEN, dtype=jnp.int32) < length
    scores = jnp.where(valid_key[None, None, :], scores, -1e+30)
    attn_probs = jnp.exp(scores - jax.nn.logsumexp(scores, -1, keepdims=True))
    context = jnp.einsum('hqk,khd->qhd', low(attn_probs), values.reshape(head_shape), precision=lax.Precision.HIGHEST).reshape(LEN, D)
    context = low(low_back(context))
    first_sum = frames_in + low_back(product(context, w_out)) + b_out
    hidden = layer_norm(first_sum, gain_one, shift_one)
    pre_act = low_back(product(low(hidden), w_up) + b_up)
    activation = low(jax.nn.gelu(pre_act, approximate=False))
    second_sum = hidden + low_back(product(activation, w_down)) + b_down
    return layer_norm(second_sum, gain_two, shift_two)

def reference(inputs, lengths, w_query, b_query, w_key, w_value, b_value, w_out, b_out, gain_one, shift_one, w_up, b_up, w_down, b_down, gain_two, shift_two, cotangent):
    params = tuple((parameter.astype(jnp.float32) for parameter in (w_query, b_query, w_key, w_value, b_value, w_out, b_out, gain_one, shift_one, w_up, b_up, w_down, b_down, gain_two, shift_two)))

    def one_clip(totals, clip_item):
        frames_in, length, grad_out = clip_item

        def forward(field, param_set):
            return clip_layer(field, length, param_set)
        result, pull_back = jax.vjp(forward, frames_in.astype(jnp.float32), params)
        grad_in, grad_params = pull_back(grad_out.astype(jnp.float32))
        totals = tuple((left_sum + right_sum for left_sum, right_sum in zip(totals, grad_params)))
        return (totals, (result.astype(jnp.bfloat16), grad_in.astype(jnp.bfloat16)))
    zero_sums = tuple((jnp.zeros_like(parameter) for parameter in params))
    totals, (output, grad_inputs) = lax.scan(one_clip, zero_sums, (inputs, lengths, cotangent))
    return (output, grad_inputs, totals[0], totals[1], totals[2], totals[3], totals[4], totals[5], totals[6], totals[7], totals[8], totals[9], totals[10], totals[11], totals[12], totals[13], totals[14])
```

```python
from functools import partial

import jax
import jax.numpy as jnp
from jax import lax
from jax.experimental import pallas as pl
from jax.experimental.pallas import tpu as pltpu
from jax.sharding import PartitionSpec as P

HEADS = 12
HD = 64
EPS = 1e-05
F32 = jnp.float32
BF16 = jnp.bfloat16


def contract(left, right, left_dim, right_dim):
    return lax.dot_general(
        left, right, (((left_dim,), (right_dim,)), ((), ())), preferred_element_type=F32
    )


def attend_kernel(len_ref, q_ref, k_ref, v_ref, o_ref, inv_ref, p_ref):
    frames = q_ref.shape[-1]
    row = lax.broadcasted_iota(jnp.int32, (16, frames), 0)
    col = lax.broadcasted_iota(jnp.int32, (16, frames), 1)
    bias = jnp.where((row == 0) & (col >= len_ref[0]), -1e30, 0.0).astype(BF16)
    one = jnp.where(row == 0, 1.0, 0.0).astype(BF16)
    keys = jnp.concatenate([k_ref[...], bias], 0)
    scaled = (q_ref[...].astype(F32) * HD ** (-0.5)).astype(BF16)
    scores = contract(keys, jnp.concatenate([scaled, one], 0), 0, 0)
    probs = jnp.exp(scores - jnp.max(scores, 0, keepdims=True))
    inverse = 1.0 / jnp.sum(probs, 0, keepdims=True)
    low_probs = probs.astype(BF16)
    o_ref[...] = (contract(v_ref[...], low_probs, 1, 0) * inverse).astype(BF16)
    inv_ref[...] = inverse
    p_ref[...] = low_probs


def attend(qkv, length):
    pieces, _, heads, _, frames = qkv.shape

    def part(which):
        return pl.BlockSpec(
            (None, None, None, HD, frames), lambda i: (i // heads, which, i % heads, 0, 0)
        )

    def out(rows):
        return pl.BlockSpec((None, None, rows, frames), lambda i: (i // heads, i % heads, 0, 0))

    shape = (pieces, heads)
    return pl.pallas_call(
        attend_kernel,
        grid=(pieces * heads,),
        out_shape=(
            jax.ShapeDtypeStruct(shape + (HD, frames), BF16),
            jax.ShapeDtypeStruct(shape + (1, frames), F32),
            jax.ShapeDtypeStruct(shape + (frames, frames), BF16),
        ),
        in_specs=[pl.BlockSpec(memory_space=pltpu.SMEM), part(0), part(1), part(2)],
        out_specs=(out(HD), out(1), out(frames)),
        compiler_params=pltpu.CompilerParams(vmem_limit_bytes=40 << 20),
        cost_estimate=pl.CostEstimate(
            flops=pieces * heads * frames * frames * 1024,
            bytes_accessed=pieces * heads * frames * frames * 2,
            transcendentals=0,
        ),
        name="attend",
    )(length, qkv, qkv, qkv)


def attend_back_kernel(q_ref, k_ref, v_ref, o_ref, inv_ref, p_ref, g_ref, out_ref):
    scaling = HD ** (-0.5)
    grad = g_ref[...].astype(F32) * inv_ref[...]
    row_dot = jnp.sum(grad * o_ref[...].astype(F32), 0, keepdims=True)
    low_grad = grad.astype(BF16)
    probs = p_ref[...]
    grad_probs = contract(v_ref[...], low_grad, 0, 0)
    grad_scores = probs * (grad_probs - row_dot).astype(BF16)
    out_ref[0] = (contract(k_ref[...], grad_scores, 1, 0) * scaling).astype(BF16)
    out_ref[1] = (contract(q_ref[...], grad_scores, 1, 1) * scaling).astype(BF16)
    out_ref[2] = contract(low_grad, probs, 1, 1).astype(BF16)


def attend_back(qkv, context, inverse, probs, grad_context):
    pieces, _, heads, _, frames = qkv.shape

    def part(which):
        return pl.BlockSpec(
            (None, None, None, HD, frames), lambda i: (i // heads, which, i % heads, 0, 0)
        )

    def one(rows):
        return pl.BlockSpec((None, None, rows, frames), lambda i: (i // heads, i % heads, 0, 0))

    return pl.pallas_call(
        attend_back_kernel,
        grid=(pieces * heads,),
        out_shape=jax.ShapeDtypeStruct(qkv.shape, BF16),
        in_specs=[part(0), part(1), part(2), one(HD), one(1), one(frames), one(HD)],
        out_specs=pl.BlockSpec(
            (None, 3, None, HD, frames), lambda i: (i // heads, 0, i % heads, 0, 0)
        ),
        compiler_params=pltpu.CompilerParams(vmem_limit_bytes=40 << 20),
        cost_estimate=pl.CostEstimate(
            flops=pieces * heads * frames * frames * 2048,
            bytes_accessed=pieces * heads * frames * frames * 2,
            transcendentals=0,
        ),
        name="attend_back",
    )(qkv, qkv, qkv, context, inverse, probs, grad_context)


def gelu_kernel(x_ref, w_ref, b_ref, act_ref, slope_ref):
    pre = contract(x_ref[...], w_ref[...], 1, 0) + b_ref[...].astype(F32)
    size = jnp.abs(pre)
    bell = jnp.exp(pre * pre * -0.5)
    t = 1.0 / (1.0 + (0.3275911 * 0.5**0.5) * size)
    series = t * (
        0.5 * 0.254829592
        + t
        * (
            0.5 * -0.284496736
            + t * (0.5 * 1.421413741 + t * (0.5 * -1.453152027 + t * (0.5 * 1.061405429)))
        )
    )
    tail = series * bell
    normal = jnp.where(pre >= 0, 1.0 - tail, tail)
    act_ref[...] = (pre * normal).astype(BF16)
    slope_ref[...] = (normal + pre * bell * (2.0 * jnp.pi) ** -0.5).astype(BF16)


def gelu_up(rows, weight, bias):
    frames, width = rows.shape
    units = weight.shape[1]
    tile = 256
    out = jax.ShapeDtypeStruct((frames, units), BF16)
    spec = pl.BlockSpec((tile, units), lambda i: (i, 0))
    return pl.pallas_call(
        gelu_kernel,
        grid=(frames // tile,),
        out_shape=(out, out),
        in_specs=[
            pl.BlockSpec((tile, width), lambda i: (i, 0)),
            pl.BlockSpec((width, units), lambda i: (0, 0)),
            pl.BlockSpec((1, units), lambda i: (0, 0)),
        ],
        out_specs=(spec, spec),
        compiler_params=pltpu.CompilerParams(vmem_limit_bytes=40 << 20),
        cost_estimate=pl.CostEstimate(
            flops=2 * frames * width * units, bytes_accessed=frames * units * 6, transcendentals=0
        ),
        name="gelu_up",
    )(rows, weight, bias)


def norm_forward(summed, gain_vec, shift_vec):
    centered = summed - jnp.mean(summed, -1, keepdims=True)
    inv_root = lax.rsqrt(jnp.mean(centered * centered, -1, keepdims=True) + EPS)
    normed = centered * inv_root
    return (normed * gain_vec + shift_vec, normed, inv_root)


def norm_backward(grad_in, normed, inv_root, gain_vec):
    scaled = grad_in * gain_vec
    return inv_root * (
        scaled
        - jnp.mean(scaled, -1, keepdims=True)
        - normed * jnp.mean(scaled * normed, -1, keepdims=True)
    )


def swap(value, axis, bit):
    return lax.ppermute(value, axis, [(i, i ^ bit) for i in range(lax.axis_size(axis))])


def bits_of(axis):
    return [1 << b for b in range(lax.axis_size(axis).bit_length() - 1)]


def gather_pieces(own):
    far = swap(own, "mp", 2)
    return [own, swap(own, "mp", 1), far, swap(far, "mp", 1)]


def add_low(left, right):
    return (left.astype(F32) + right.astype(F32)).astype(left.dtype)


def scatter_pieces(pieces):
    far = add_low(pieces[2], swap(pieces[3], "mp", 1))
    near = add_low(pieces[0], swap(pieces[1], "mp", 1))
    return add_low(near, swap(far, "mp", 2))


def reduce_all(value):
    index = lax.axis_index("dp")
    for bit in bits_of("dp"):
        mine = (index // bit) % 2
        half = value.shape[0] // 2
        sent = lax.dynamic_slice_in_dim(value, (1 - mine) * half, half, 0)
        kept = lax.dynamic_slice_in_dim(value, mine * half, half, 0)
        value = add_low(kept, swap(sent, "dp", bit))
    for bit in reversed(bits_of("dp")):
        low_side = (index // bit) % 2 == 0
        other = swap(value, "dp", bit)
        value = jnp.concatenate(
            [jnp.where(low_side, value, other), jnp.where(low_side, other, value)], 0
        )
    return value


def reduce_small(value, axes):
    for axis in axes:
        for bit in bits_of(axis):
            value = value + swap(value, axis, bit)
    return value


def per_device(
    inputs,
    lengths,
    w_query,
    b_query,
    w_key,
    w_value,
    b_value,
    w_out,
    b_out,
    gain_one,
    shift_one,
    w_up,
    b_up,
    w_down,
    b_down,
    gain_two,
    shift_two,
    cotangent,
):
    own_clips, frames, width = inputs.shape
    part_cols = w_query.shape[1]
    part_heads = part_cols // HD
    rows_in = inputs.reshape(own_clips * frames, width)
    length = lax.dynamic_slice_in_dim(lengths, lax.axis_index("mp") * own_clips, own_clips, 0)

    w_attn = gather_pieces(jnp.concatenate([w_query.T, w_key.T, w_value.T], 0))
    biases = gather_pieces(
        jnp.concatenate([b_query, jnp.zeros_like(b_query), b_value, b_up], 0).reshape(1, -1)
    )
    w_outs = gather_pieces(w_out)
    w_ups = gather_pieces(w_up)
    w_downs = gather_pieces(w_down)

    held = []
    for pair in (0, 2):
        weight = jnp.concatenate(w_attn[pair : pair + 2], 0)
        bias = jnp.concatenate([b[0, : 3 * part_cols] for b in biases[pair : pair + 2]], 0)
        qkv = (contract(weight, rows_in, 1, 1) + bias.astype(F32)[:, None]).astype(BF16)
        qkv = qkv.reshape(2, 3, part_heads, HD, frames)
        held.append((qkv,) + tuple(attend(qkv, length)))
    context = jnp.concatenate([h[1].reshape(2 * part_cols, frames) for h in held], 0)
    w_out_all = jnp.concatenate(w_outs, 0)
    first_sum = (
        rows_in.astype(F32) + contract(context, w_out_all, 0, 0) + b_out.astype(F32)
    )
    gain_one, gain_two = gain_one.astype(F32), gain_two.astype(F32)
    hidden, normed_one, inv_one = norm_forward(first_sum, gain_one, shift_one.astype(F32))
    low_hidden = hidden.astype(BF16)

    ups = [gelu_up(low_hidden, w_ups[r], biases[r][:, 3 * part_cols :]) for r in range(4)]
    ffn_sum = sum(contract(ups[r][0], w_downs[r], 1, 0) for r in range(4))
    second_sum = hidden + ffn_sum + b_down.astype(F32)
    output, normed_two, inv_two = norm_forward(second_sum, gain_two, shift_two.astype(F32))
    grad_out = cotangent.reshape(own_clips * frames, width).astype(F32)
    grad_two = norm_backward(grad_out, normed_two, inv_two, gain_two)
    low_two = grad_two.astype(BF16)

    grad_w_down, grad_w_up, grad_b_up = [None] * 4, [None] * 4, [None] * 4
    back = 0
    grad_pre = [None] * 4
    for r in (3, 2, 1, 0):
        act, slope = ups[r]
        grad_w_down[r] = contract(act, low_two, 0, 0).astype(BF16)
    g_down = reduce_all(scatter_pieces(grad_w_down))
    for r in (3, 2, 1, 0):
        act, slope = ups[r]
        grad_pre[r] = (contract(low_two, w_downs[r], 1, 1) * slope.astype(F32)).astype(BF16)
        grad_w_up[r] = contract(low_hidden, grad_pre[r], 0, 0).astype(BF16)
        grad_b_up[r] = jnp.sum(grad_pre[r].astype(F32), 0)
        back = back + contract(grad_pre[r], w_ups[r], 1, 1)
    g_up = reduce_all(scatter_pieces(grad_w_up))
    grad_hidden = grad_two + back
    grad_one = norm_backward(grad_hidden, normed_one, inv_one, gain_one)
    low_one = grad_one.astype(BF16)
    whole = jnp.stack(
        [
            jnp.sum(grad_one, 0),
            jnp.sum(grad_hidden * normed_one, 0),
            jnp.sum(grad_hidden, 0),
            jnp.sum(grad_two, 0),
            jnp.sum(grad_out * normed_two, 0),
            jnp.sum(grad_out, 0),
        ]
    )
    whole = reduce_small(whole, ("mp", "dp"))

    grad_context = contract(w_out_all, low_one, 1, 1).astype(BF16)
    grad_w_out = contract(context, low_one, 1, 0).astype(BF16).reshape(4, part_cols, width)
    g_out = reduce_all(scatter_pieces([grad_w_out[r] for r in range(4)]))
    grad_context = grad_context.reshape(4, part_heads, HD, frames)
    grad_attn, grad_b_attn, grad_x = [None] * 4, [None] * 4, grad_one
    for pair in (2, 0):
        qkv, ctx, inverse, probs = held[pair // 2]
        grads = attend_back(qkv, ctx, inverse, probs, grad_context[pair : pair + 2])
        grads = grads.reshape(2 * 3 * part_cols, frames)
        weight = jnp.concatenate(w_attn[pair : pair + 2], 0)
        grad_w = contract(grads, rows_in, 1, 0).astype(BF16).reshape(2, 3 * part_cols, width)
        grad_b = jnp.sum(grads.astype(F32), 1).reshape(2, 3 * part_cols)
        for k in range(2):
            grad_attn[pair + k] = grad_w[k]
            grad_b_attn[pair + k] = grad_b[k]
        grad_x = grad_x + contract(grads, weight, 0, 0)
    g_attn = reduce_all(scatter_pieces(grad_attn)).astype(F32)
    g_bias = reduce_small(
        scatter_pieces(
            [jnp.concatenate([grad_b_attn[r], grad_b_up[r]])[None] for r in range(4)]
        ),
        ("dp",),
    )[0]
    grad_inputs = grad_x.astype(BF16).reshape(inputs.shape)
    cols = part_cols
    return (
        output.astype(BF16).reshape(inputs.shape),
        grad_inputs,
        g_attn[:cols].T,
        g_bias[:cols],
        g_attn[cols : 2 * cols].T,
        g_attn[2 * cols : 3 * cols].T,
        g_bias[2 * cols : 3 * cols],
        g_out.astype(F32),
        whole[0],
        whole[1],
        whole[2],
        g_up.astype(F32),
        g_bias[3 * cols :],
        g_down.astype(F32),
        whole[3],
        whole[4],
        whole[5],
    )


def solution(mesh):
    clips = P(("dp", "mp"), None, None)
    placed = (
        clips,
        P("dp"),
        P(None, "mp"),
        P("mp"),
        P(None, "mp"),
        P(None, "mp"),
        P("mp"),
        P("mp", None),
        P(),
        P(),
        P(),
        P(None, "mp"),
        P("mp"),
        P("mp", None),
        P(),
        P(),
        P(),
        clips,
    )
    return jax.shard_map(
        per_device,
        mesh=mesh,
        in_specs=placed,
        out_specs=(clips, clips) + placed[2:17],
        check_vma=False,
    )
```

```python
import jax
import jax.numpy as jnp
from jax import lax
from jax.experimental import pallas as pl
from jax.experimental.pallas import tpu as pltpu
from jax.sharding import PartitionSpec as P


HD = 64
EPS = 1e-05
F32 = jnp.float32
BF16 = jnp.bfloat16


def contract(left, right, left_dim, right_dim):
    return lax.dot_general(
        left, right, (((left_dim,), (right_dim,)), ((), ())), preferred_element_type=F32
    )


def attend_kernel(len_ref, q_ref, k_ref, v_ref, o_ref, inv_ref, p_ref):
    frames = q_ref.shape[-1]
    row = lax.broadcasted_iota(jnp.int32, (16, frames), 0)
    col = lax.broadcasted_iota(jnp.int32, (16, frames), 1)
    bias = jnp.where((row == 0) & (col >= len_ref[0]), -1e30, 0.0).astype(BF16)
    one = jnp.where(row == 0, 1.0, 0.0).astype(BF16)
    keys = jnp.concatenate([k_ref[...], bias], 0)
    scaled = (q_ref[...].astype(F32) * HD ** (-0.5)).astype(BF16)
    scores = contract(keys, jnp.concatenate([scaled, one], 0), 0, 0)
    probs = jnp.exp(scores - jnp.max(scores, 0, keepdims=True))
    inverse = 1.0 / jnp.sum(probs, 0, keepdims=True)
    low_probs = probs.astype(BF16)
    o_ref[...] = (contract(v_ref[...], low_probs, 1, 0) * inverse).astype(BF16)
    inv_ref[...] = inverse
    p_ref[...] = low_probs


def attend(qkv, length):
    pieces, _, heads, _, frames = qkv.shape

    def part(which):
        return pl.BlockSpec(
            (None, None, None, HD, frames), lambda i: (i // heads, which, i % heads, 0, 0)
        )

    def out(rows):
        return pl.BlockSpec((None, None, rows, frames), lambda i: (i // heads, i % heads, 0, 0))

    shape = (pieces, heads)
    return pl.pallas_call(
        attend_kernel,
        grid=(pieces * heads,),
        out_shape=(
            jax.ShapeDtypeStruct(shape + (HD, frames), BF16),
            jax.ShapeDtypeStruct(shape + (1, frames), F32),
            jax.ShapeDtypeStruct(shape + (frames, frames), BF16),
        ),
        in_specs=[pl.BlockSpec(memory_space=pltpu.SMEM), part(0), part(1), part(2)],
        out_specs=(out(HD), out(1), out(frames)),
        compiler_params=pltpu.CompilerParams(vmem_limit_bytes=40 << 20),
        cost_estimate=pl.CostEstimate(
            flops=pieces * heads * frames * frames * 1024,
            bytes_accessed=pieces * heads * frames * frames * 2,
            transcendentals=0,
        ),
        name="attend",
    )(length, qkv, qkv, qkv)


def attend_back_kernel(q_ref, k_ref, v_ref, o_ref, inv_ref, p_ref, g_ref, out_ref):
    scaling = HD ** (-0.5)
    grad = g_ref[...].astype(F32) * inv_ref[...]
    row_dot = jnp.sum(grad * o_ref[...].astype(F32), 0, keepdims=True)
    low_grad = grad.astype(BF16)
    probs = p_ref[...]
    grad_probs = contract(v_ref[...], low_grad, 0, 0)
    grad_scores = probs * (grad_probs - row_dot).astype(BF16)
    out_ref[0] = (contract(k_ref[...], grad_scores, 1, 0) * scaling).astype(BF16)
    out_ref[1] = (contract(q_ref[...], grad_scores, 1, 1) * scaling).astype(BF16)
    out_ref[2] = contract(low_grad, probs, 1, 1).astype(BF16)


def attend_back(qkv, context, inverse, probs, grad_context):
    pieces, _, heads, _, frames = qkv.shape

    def part(which):
        return pl.BlockSpec(
            (None, None, None, HD, frames), lambda i: (i // heads, which, i % heads, 0, 0)
        )

    def one(rows):
        return pl.BlockSpec((None, None, rows, frames), lambda i: (i // heads, i % heads, 0, 0))

    return pl.pallas_call(
        attend_back_kernel,
        grid=(pieces * heads,),
        out_shape=jax.ShapeDtypeStruct(qkv.shape, BF16),
        in_specs=[part(0), part(1), part(2), one(HD), one(1), one(frames), one(HD)],
        out_specs=pl.BlockSpec(
            (None, 3, None, HD, frames), lambda i: (i // heads, 0, i % heads, 0, 0)
        ),
        compiler_params=pltpu.CompilerParams(vmem_limit_bytes=40 << 20),
        cost_estimate=pl.CostEstimate(
            flops=pieces * heads * frames * frames * 2048,
            bytes_accessed=pieces * heads * frames * frames * 2,
            transcendentals=0,
        ),
        name="attend_back",
    )(qkv, qkv, qkv, context, inverse, probs, grad_context)


def gelu_kernel(x_ref, w_ref, b_ref, act_ref, slope_ref):
    pre = contract(x_ref[...], w_ref[...], 1, 0) + b_ref[...].astype(F32)
    size = jnp.abs(pre)
    bell = jnp.exp(pre * pre * -0.5)
    t = 1.0 / (1.0 + (0.3275911 * 0.5**0.5) * size)
    series = t * (
        0.5 * 0.254829592
        + t
        * (
            0.5 * -0.284496736
            + t * (0.5 * 1.421413741 + t * (0.5 * -1.453152027 + t * (0.5 * 1.061405429)))
        )
    )
    tail = series * bell
    normal = jnp.where(pre >= 0, 1.0 - tail, tail)
    act_ref[...] = (pre * normal).astype(BF16)
    slope_ref[...] = (normal + pre * bell * (2.0 * jnp.pi) ** -0.5).astype(BF16)


def gelu_up(rows, weight, bias):
    frames, width = rows.shape
    units = weight.shape[1]
    tile = 256
    out = jax.ShapeDtypeStruct((frames, units), BF16)
    spec = pl.BlockSpec((tile, units), lambda i: (i, 0))
    return pl.pallas_call(
        gelu_kernel,
        grid=(frames // tile,),
        out_shape=(out, out),
        in_specs=[
            pl.BlockSpec((tile, width), lambda i: (i, 0)),
            pl.BlockSpec((width, units), lambda i: (0, 0)),
            pl.BlockSpec((1, units), lambda i: (0, 0)),
        ],
        out_specs=(spec, spec),
        compiler_params=pltpu.CompilerParams(vmem_limit_bytes=40 << 20),
        cost_estimate=pl.CostEstimate(
            flops=2 * frames * width * units, bytes_accessed=frames * units * 6, transcendentals=0
        ),
        name="gelu_up",
    )(rows, weight, bias)


def norm_forward(summed, gain_vec, shift_vec):
    centered = summed - jnp.mean(summed, -1, keepdims=True)
    inv_root = lax.rsqrt(jnp.mean(centered * centered, -1, keepdims=True) + EPS)
    normed = centered * inv_root
    return (normed * gain_vec + shift_vec, normed, inv_root)


def norm_backward(grad_in, normed, inv_root, gain_vec):
    scaled = grad_in * gain_vec
    return inv_root * (
        scaled
        - jnp.mean(scaled, -1, keepdims=True)
        - normed * jnp.mean(scaled * normed, -1, keepdims=True)
    )


def swap(value, axis, bit):
    return lax.ppermute(value, axis, [(i, i ^ bit) for i in range(lax.axis_size(axis))])


def bits_of(axis):
    return [1 << b for b in range(lax.axis_size(axis).bit_length() - 1)]


def add_low(left, right):
    return (left.astype(F32) + right.astype(F32)).astype(left.dtype)


def scatter_near(far, near, near_other):
    near = add_low(near, swap(near_other, "mp", 1))
    return add_low(near, swap(far, "mp", 2))


def reduce_all(value, order):
    index = lax.axis_index("dp")
    for bit in order:
        mine = (index // bit) % 2
        half = value.shape[0] // 2
        sent = lax.dynamic_slice_in_dim(value, (1 - mine) * half, half, 0)
        kept = lax.dynamic_slice_in_dim(value, mine * half, half, 0)
        value = add_low(kept, swap(sent, "dp", bit))
    for bit in reversed(order):
        low_side = (index // bit) % 2 == 0
        other = swap(value, "dp", bit)
        value = jnp.concatenate(
            [jnp.where(low_side, value, other), jnp.where(low_side, other, value)], 0
        )
    return value


def reduce_small(whole, pieces):
    for bit in bits_of("mp"):
        rows = [r ^ bit for r in range(pieces.shape[0])]
        flat = jnp.concatenate([whole.reshape(-1), pieces.reshape(-1)])
        other = swap(flat, "mp", bit)
        whole = whole + other[: whole.size].reshape(whole.shape)
        other = other[whole.size :].reshape(pieces.shape)
        pieces = pieces + jnp.stack([other[r] for r in rows])
    flat = jnp.concatenate([whole.reshape(-1), pieces[0]])
    for bit in bits_of("dp"):
        flat = flat + swap(flat, "dp", bit)
    return flat[: whole.size].reshape(whole.shape), flat[whole.size :]


def per_device(
    inputs,
    lengths,
    w_query,
    b_query,
    w_key,
    w_value,
    b_value,
    w_out,
    b_out,
    gain_one,
    shift_one,
    w_up,
    b_up,
    w_down,
    b_down,
    gain_two,
    shift_two,
    cotangent,
):
    own_clips, frames, width = inputs.shape
    part_cols = w_query.shape[1]
    part_heads = part_cols // HD
    rows_in = inputs.reshape(own_clips * frames, width)
    length = lax.dynamic_slice_in_dim(lengths, lax.axis_index("mp") * own_clips, own_clips, 0)

    def gather(own):
        far = swap(own, "mp", 2)
        return [own, swap(own, "mp", 1), far, swap(far, "mp", 1)]

    w_attn = gather(jnp.concatenate([w_query.T, w_key.T, w_value.T], 0))
    biases = gather(
        jnp.concatenate([b_query, jnp.zeros_like(b_query), b_value, b_up], 0).reshape(1, -1)
    )
    w_outs = gather(w_out)
    w_ups = gather(w_up)
    w_downs = gather(w_down)

    held = []
    for r in range(4):
        bias = biases[r][0, : 3 * part_cols].astype(F32)[:, None]
        qkv = (contract(w_attn[r], rows_in, 1, 1) + bias).astype(BF16)
        qkv = qkv.reshape(1, 3, part_heads, HD, frames)
        held.append((qkv,) + tuple(attend(qkv, length)))
    context = jnp.concatenate([h[1].reshape(part_cols, frames) for h in held], 0)
    w_out_all = jnp.concatenate(w_outs, 0)
    mixed = contract(context, w_out_all, 0, 0)
    first_sum = rows_in.astype(F32) + mixed + b_out.astype(F32)
    gain_one, gain_two = gain_one.astype(F32), gain_two.astype(F32)
    hidden, normed_one, inv_one = norm_forward(first_sum, gain_one, shift_one.astype(F32))
    low_hidden = hidden.astype(BF16)

    ups = []
    for r in range(4):
        ups.append(gelu_up(low_hidden, w_ups[r], biases[r][:, 3 * part_cols :]))
    ffn_sum = 0
    for r in range(4):
        ffn_sum = ffn_sum + contract(ups[r][0], w_downs[r], 1, 0)
    second_sum = hidden + ffn_sum + b_down.astype(F32)
    output, normed_two, inv_two = norm_forward(second_sum, gain_two, shift_two.astype(F32))
    grad_out = cotangent.reshape(own_clips * frames, width).astype(F32)
    grad_two = norm_backward(grad_out, normed_two, inv_two, gain_two)
    low_two = grad_two.astype(BF16)

    grad_w_down, grad_w_up, grad_b_up = [None] * 4, [None] * 4, [None] * 4
    grad_pre = [None] * 4
    for r in (3, 2, 1, 0):
        grad_w_down[r] = contract(ups[r][0], low_two, 0, 0).astype(BF16)
    far = add_low(grad_w_down[2], swap(grad_w_down[3], "mp", 1))
    own = scatter_near(far, grad_w_down[0], grad_w_down[1])
    g_down = reduce_all(own, bits_of("dp"))
    back = 0
    for r in (3, 2, 1, 0):
        grad_pre[r] = (contract(low_two, w_downs[r], 1, 1) * ups[r][1].astype(F32)).astype(BF16)
        grad_b_up[r] = jnp.sum(grad_pre[r].astype(F32), 0)
        grad_w_up[r] = contract(low_hidden, grad_pre[r], 0, 0).astype(BF16)
    for r in (3, 2, 1, 0):
        back = back + contract(grad_pre[r], w_ups[r], 1, 1)
    far = add_low(grad_w_up[2], swap(grad_w_up[3], "mp", 1))
    own = scatter_near(far, grad_w_up[0], grad_w_up[1])
    g_up = reduce_all(own, bits_of("dp"))
    grad_hidden = grad_two + back
    grad_one = norm_backward(grad_hidden, normed_one, inv_one, gain_one)
    low_one = grad_one.astype(BF16)
    whole = jnp.stack(
        [
            jnp.sum(grad_one, 0),
            jnp.sum(grad_hidden * normed_one, 0),
            jnp.sum(grad_hidden, 0),
            jnp.sum(grad_two, 0),
            jnp.sum(grad_out * normed_two, 0),
            jnp.sum(grad_out, 0),
        ]
    )

    grad_context = contract(w_out_all, low_one, 1, 1).astype(BF16)
    grad_w_out = contract(context, low_one, 1, 0).astype(BF16).reshape(4, part_cols, width)
    grad_context = grad_context.reshape(4, 1, part_heads, HD, frames)
    grad_attn, grad_b_attn, grad_x = [None] * 4, [None] * 4, grad_one
    for r in (3, 2, 1, 0):
        qkv, ctx, inverse, probs = held[r]
        grads = attend_back(qkv, ctx, inverse, probs, grad_context[r])
        grads = grads.reshape(3 * part_cols, frames)
        grad_w = contract(grads, rows_in, 1, 0).astype(BF16)
        grad_attn[r] = jnp.concatenate([grad_w, grad_w_out[r]], 0)
        grad_b_attn[r] = jnp.sum(grads.astype(F32), 1)
        grad_x = grad_x + contract(grads, w_attn[r], 0, 0)
    far = add_low(grad_attn[2], swap(grad_attn[3], "mp", 1))
    own = scatter_near(far, grad_attn[0], grad_attn[1])
    split = own.shape[0] // 2
    order = bits_of("dp")
    g_attn = jnp.concatenate(
        [reduce_all(own[:split], order), reduce_all(own[split:], order[1:] + order[:1])],
        0,
    ).astype(F32)
    whole, g_bias = reduce_small(
        whole, jnp.stack([jnp.concatenate([grad_b_attn[r], grad_b_up[r]]) for r in range(4)])
    )
    grad_inputs = grad_x.astype(BF16).reshape(inputs.shape)
    cols = part_cols
    return (
        output.astype(BF16).reshape(inputs.shape),
        grad_inputs,
        g_attn[:cols].T,
        g_bias[:cols],
        g_attn[cols : 2 * cols].T,
        g_attn[2 * cols : 3 * cols].T,
        g_bias[2 * cols : 3 * cols],
        g_attn[3 * cols :],
        whole[0],
        whole[1],
        whole[2],
        g_up.astype(F32),
        g_bias[3 * cols :],
        g_down.astype(F32),
        whole[3],
        whole[4],
        whole[5],
    )


def solution(mesh):
    clips = P(("dp", "mp"), None, None)
    placed = (
        clips,
        P("dp"),
        P(None, "mp"),
        P("mp"),
        P(None, "mp"),
        P(None, "mp"),
        P("mp"),
        P("mp", None),
        P(),
        P(),
        P(),
        P(None, "mp"),
        P("mp"),
        P("mp", None),
        P(),
        P(),
        P(),
        clips,
    )
    return jax.shard_map(
        per_device,
        mesh=mesh,
        in_specs=placed,
        out_specs=(clips, clips) + placed[2:17],
        check_vma=False,
    )
```

```python
import jax
import jax.numpy as jnp
from jax import lax
from jax.experimental import pallas as pl
from jax.experimental.pallas import tpu as pltpu
from jax.sharding import PartitionSpec as P


HD = 64
EPS = 1e-05
F32 = jnp.float32
BF16 = jnp.bfloat16


def contract(left, right, left_dim, right_dim):
    return lax.dot_general(
        left, right, (((left_dim,), (right_dim,)), ((), ())), preferred_element_type=F32
    )


def attend_kernel(len_ref, q_ref, k_ref, v_ref, o_ref, inv_ref, p_ref):
    frames = q_ref.shape[-1]
    row = lax.broadcasted_iota(jnp.int32, (16, frames), 0)
    col = lax.broadcasted_iota(jnp.int32, (16, frames), 1)
    bias = jnp.where((row == 0) & (col >= len_ref[0]), -1e30, 0.0).astype(BF16)
    one = jnp.where(row == 0, 1.0, 0.0).astype(BF16)
    keys = jnp.concatenate([k_ref[...], bias], 0)
    scaled = (q_ref[...].astype(F32) * HD ** (-0.5)).astype(BF16)
    scores = contract(keys, jnp.concatenate([scaled, one], 0), 0, 0)
    probs = jnp.exp(scores - jnp.max(scores, 0, keepdims=True))
    inverse = 1.0 / jnp.sum(probs, 0, keepdims=True)
    low_probs = probs.astype(BF16)
    o_ref[...] = (contract(v_ref[...], low_probs, 1, 0) * inverse).astype(BF16)
    inv_ref[...] = inverse
    p_ref[...] = low_probs


def in_hbm(value):
    return pltpu.with_memory_space_constraint(value, pltpu.MemorySpace.HBM)


def attend(qkv, length):
    pieces, _, heads, _, frames = qkv.shape

    def part(which):
        return pl.BlockSpec(
            (None, None, None, HD, frames), lambda i: (i // heads, which, i % heads, 0, 0)
        )

    def out(rows):
        return pl.BlockSpec((None, None, rows, frames), lambda i: (i // heads, i % heads, 0, 0))

    shape = (pieces, heads)
    return pl.pallas_call(
        attend_kernel,
        grid=(pieces * heads,),
        out_shape=(
            jax.ShapeDtypeStruct(shape + (HD, frames), BF16),
            jax.ShapeDtypeStruct(shape + (1, frames), F32),
            pltpu.HBM(shape + (frames, frames), BF16),
        ),
        in_specs=[pl.BlockSpec(memory_space=pltpu.SMEM), part(0), part(1), part(2)],
        out_specs=(out(HD), out(1), out(frames)),
        compiler_params=pltpu.CompilerParams(vmem_limit_bytes=40 << 20),
        cost_estimate=pl.CostEstimate(
            flops=pieces * heads * frames * frames * 1024,
            bytes_accessed=pieces * heads * frames * frames * 2,
            transcendentals=0,
        ),
        name="attend",
    )(length, qkv, qkv, qkv)


def attend_back_kernel(q_ref, k_ref, v_ref, o_ref, inv_ref, p_ref, g_ref, out_ref):
    scaling = HD ** (-0.5)
    grad = g_ref[...].astype(F32) * inv_ref[...]
    row_dot = jnp.sum(grad * o_ref[...].astype(F32), 0, keepdims=True)
    low_grad = grad.astype(BF16)
    probs = p_ref[...]
    grad_probs = contract(v_ref[...], low_grad, 0, 0)
    grad_scores = probs * (grad_probs - row_dot).astype(BF16)
    out_ref[0] = (contract(k_ref[...], grad_scores, 1, 0) * scaling).astype(BF16)
    out_ref[1] = (contract(q_ref[...], grad_scores, 1, 1) * scaling).astype(BF16)
    out_ref[2] = contract(low_grad, probs, 1, 1).astype(BF16)


def attend_back(qkv, context, inverse, probs, grad_context):
    pieces, _, heads, _, frames = qkv.shape

    def part(which):
        return pl.BlockSpec(
            (None, None, None, HD, frames), lambda i: (i // heads, which, i % heads, 0, 0)
        )

    def one(rows):
        return pl.BlockSpec((None, None, rows, frames), lambda i: (i // heads, i % heads, 0, 0))

    return pl.pallas_call(
        attend_back_kernel,
        grid=(pieces * heads,),
        out_shape=jax.ShapeDtypeStruct(qkv.shape, BF16),
        in_specs=[part(0), part(1), part(2), one(HD), one(1), one(frames), one(HD)],
        out_specs=pl.BlockSpec(
            (None, 3, None, HD, frames), lambda i: (i // heads, 0, i % heads, 0, 0)
        ),
        compiler_params=pltpu.CompilerParams(vmem_limit_bytes=40 << 20),
        cost_estimate=pl.CostEstimate(
            flops=pieces * heads * frames * frames * 2048,
            bytes_accessed=pieces * heads * frames * frames * 2,
            transcendentals=0,
        ),
        name="attend_back",
    )(qkv, qkv, qkv, context, inverse, probs, grad_context)


def gelu_kernel(x_ref, w_ref, b_ref, act_ref, slope_ref):
    pre = contract(x_ref[...], w_ref[...], 1, 0) + b_ref[...].astype(F32)
    size = jnp.abs(pre)
    bell = jnp.exp(pre * pre * -0.5)
    t = 1.0 / (1.0 + (0.3275911 * 0.5**0.5) * size)
    series = t * (
        0.5 * 0.254829592
        + t
        * (
            0.5 * -0.284496736
            + t * (0.5 * 1.421413741 + t * (0.5 * -1.453152027 + t * (0.5 * 1.061405429)))
        )
    )
    tail = series * bell
    normal = jnp.where(pre >= 0, 1.0 - tail, tail)
    act_ref[...] = (pre * normal).astype(BF16)
    slope_ref[...] = (normal + pre * bell * (2.0 * jnp.pi) ** -0.5).astype(BF16)


def gelu_up(rows, weight, bias):
    frames, width = rows.shape
    units = weight.shape[1]
    tile = 256
    out = jax.ShapeDtypeStruct((frames, units), BF16)
    spec = pl.BlockSpec((tile, units), lambda i: (i, 0))
    return pl.pallas_call(
        gelu_kernel,
        grid=(frames // tile,),
        out_shape=(out, out),
        in_specs=[
            pl.BlockSpec((tile, width), lambda i: (i, 0)),
            pl.BlockSpec((width, units), lambda i: (0, 0)),
            pl.BlockSpec((1, units), lambda i: (0, 0)),
        ],
        out_specs=(spec, spec),
        compiler_params=pltpu.CompilerParams(vmem_limit_bytes=40 << 20),
        cost_estimate=pl.CostEstimate(
            flops=2 * frames * width * units, bytes_accessed=frames * units * 6, transcendentals=0
        ),
        name="gelu_up",
    )(rows, weight, bias)


def norm_forward(summed, gain_vec, shift_vec):
    centered = summed - jnp.mean(summed, -1, keepdims=True)
    inv_root = lax.rsqrt(jnp.mean(centered * centered, -1, keepdims=True) + EPS)
    normed = centered * inv_root
    return (normed * gain_vec + shift_vec, normed, inv_root)


def norm_backward(grad_in, normed, inv_root, gain_vec):
    scaled = grad_in * gain_vec
    return inv_root * (
        scaled
        - jnp.mean(scaled, -1, keepdims=True)
        - normed * jnp.mean(scaled * normed, -1, keepdims=True)
    )


def swap(value, axis, bit):
    return lax.ppermute(value, axis, [(i, i ^ bit) for i in range(lax.axis_size(axis))])


def bits_of(axis):
    return [1 << b for b in range(lax.axis_size(axis).bit_length() - 1)]


def add_low(left, right):
    return (left.astype(F32) + right.astype(F32)).astype(left.dtype)


def scatter_near(far, near, near_other):
    near = add_low(near, swap(near_other, "mp", 1))
    return add_low(near, swap(far, "mp", 2))


def reduce_all(value, order):
    index = lax.axis_index("dp")
    for bit in order:
        mine = (index // bit) % 2
        half = value.shape[0] // 2
        sent = lax.dynamic_slice_in_dim(value, (1 - mine) * half, half, 0)
        kept = lax.dynamic_slice_in_dim(value, mine * half, half, 0)
        value = add_low(kept, swap(sent, "dp", bit))
    for bit in reversed(order):
        low_side = (index // bit) % 2 == 0
        other = swap(value, "dp", bit)
        value = jnp.concatenate(
            [jnp.where(low_side, value, other), jnp.where(low_side, other, value)], 0
        )
    return value


def reduce_small(groups):
    for bit in bits_of("mp"):
        other = swap(groups, "mp", bit)
        groups = groups + jnp.concatenate([other[r ^ bit][None] for r in range(4)], 0)
    own = lax.broadcasted_iota(jnp.int32, groups.shape[1:], 0) < 2
    value = jnp.where(own, groups[0], jnp.sum(groups, 0))
    for bit in bits_of("dp"):
        value = value + swap(value, "dp", bit)
    return value


def finish_kernel(*refs):
    grads, weights, rows = refs[:4], refs[4:8], refs[8:18]
    base_ref, out_ref, sums_ref = refs[18:]
    cols = grads[0].shape[0]
    tile = grads[0].shape[1]

    @pl.when(pl.program_id(0) == 0)
    def _():
        sums_ref[...] = jnp.zeros(sums_ref.shape, F32)
        for r in range(4):
            sums_ref[r, 1:2, :] = rows[r][...]
        for k in range(6):
            sums_ref[0, 2 + k : 3 + k, :] = rows[4 + k][...]

    total = base_ref[...]
    ones = jnp.full((8, tile), 1.0, BF16)
    for r in range(4):
        piece = grads[r][...]
        total = total + contract(piece, weights[r][...], 0, 0)
        sums_ref[r, 0:1, :cols] += contract(ones, piece, 1, 1)[0:1]
    out_ref[...] = total.astype(BF16)


def finish(grads, weights, rows, base):
    frames, width = base.shape
    cols = grads[0].shape[0]
    tile = 256
    return pl.pallas_call(
        finish_kernel,
        grid=(frames // tile,),
        out_shape=(
            jax.ShapeDtypeStruct((frames, width), BF16),
            jax.ShapeDtypeStruct((4, 8, width), F32),
        ),
        in_specs=[pl.BlockSpec((cols, tile), lambda i: (0, i))] * 4
        + [pl.BlockSpec((cols, width), lambda i: (0, 0))] * 4
        + [pl.BlockSpec((1, width), lambda i: (0, 0))] * 10
        + [pl.BlockSpec((tile, width), lambda i: (i, 0))],
        out_specs=(
            pl.BlockSpec((tile, width), lambda i: (i, 0)),
            pl.BlockSpec((4, 8, width), lambda i: (0, 0, 0)),
        ),
        compiler_params=pltpu.CompilerParams(vmem_limit_bytes=40 << 20),
        cost_estimate=pl.CostEstimate(
            flops=8 * frames * width * cols, bytes_accessed=frames * width * 12, transcendentals=0
        ),
        name="finish",
    )(*grads, *weights, *rows, base)


def per_device(
    inputs,
    lengths,
    w_query,
    b_query,
    w_key,
    w_value,
    b_value,
    w_out,
    b_out,
    gain_one,
    shift_one,
    w_up,
    b_up,
    w_down,
    b_down,
    gain_two,
    shift_two,
    cotangent,
):
    own_clips, frames, width = inputs.shape
    part_cols = w_query.shape[1]
    part_heads = part_cols // HD
    rows_in = inputs.reshape(own_clips * frames, width)
    length = lax.dynamic_slice_in_dim(lengths, lax.axis_index("mp") * own_clips, own_clips, 0)

    def gather(own):
        far = swap(own, "mp", 2)
        return [own, swap(own, "mp", 1), far, swap(far, "mp", 1)]

    w_attn = gather(jnp.concatenate([w_query.T, w_key.T, w_value.T], 0))
    biases = gather(
        jnp.concatenate([b_query, jnp.zeros_like(b_query), b_value, b_up], 0).reshape(1, -1)
    )
    w_outs = gather(w_out)

    def gather_halves(own):
        half = own.shape[0] // 2
        side = lax.axis_index("dp") % 2
        got = swap(lax.dynamic_slice_in_dim(own, side * half, half, 0), "mp", 2)
        other = swap(got, "dp", 1)
        low = side == 0
        far = jnp.concatenate([jnp.where(low, got, other), jnp.where(low, other, got)], 0)
        return [own, swap(own, "mp", 1), far, swap(far, "mp", 1)]

    w_ups = gather_halves(w_up)
    w_downs = gather_halves(w_down)
    vectors = jnp.stack([b_out, gain_one, shift_one, b_down, gain_two, shift_two]).astype(F32)
    b_out, gain_one, shift_one, b_down, gain_two, shift_two = [vectors[k : k + 1] for k in range(6)]

    held = []
    for r in range(4):
        bias = biases[r][0, : 3 * part_cols].astype(F32)[:, None]
        qkv = (contract(w_attn[r], rows_in, 1, 1) + bias).astype(BF16)
        qkv = qkv.reshape(1, 3, part_heads, HD, frames)
        ctx, inverse, probs = attend(qkv, length)
        held.append((qkv, ctx, inverse, in_hbm(probs)))
    context = jnp.concatenate([h[1].reshape(part_cols, frames) for h in held], 0)
    w_out_all = jnp.concatenate(w_outs, 0)
    mixed = contract(context, w_out_all, 0, 0)
    first_sum = rows_in.astype(F32) + mixed + b_out
    hidden, normed_one, inv_one = norm_forward(first_sum, gain_one, shift_one)
    low_hidden = hidden.astype(BF16)

    ups = []
    for r in range(4):
        ups.append(gelu_up(low_hidden, w_ups[r], biases[r][:, 3 * part_cols :]))
    ffn_sum = 0
    for r in range(4):
        ffn_sum = ffn_sum + contract(ups[r][0], w_downs[r], 1, 0)
    second_sum = hidden + ffn_sum + b_down
    output, normed_two, inv_two = norm_forward(second_sum, gain_two, shift_two)
    grad_out = cotangent.reshape(own_clips * frames, width).astype(F32)
    grad_two = norm_backward(grad_out, normed_two, inv_two, gain_two)
    low_two = grad_two.astype(BF16)

    grad_w_down, grad_w_up, grad_b_up = [None] * 4, [None] * 4, [None] * 4
    grad_pre = [None] * 4
    for r in (3, 2, 1, 0):
        grad_w_down[r] = contract(ups[r][0], low_two, 0, 0).astype(BF16)
    far = add_low(grad_w_down[2], swap(grad_w_down[3], "mp", 1))
    own = scatter_near(far, grad_w_down[0], grad_w_down[1])
    g_down = reduce_all(own, bits_of("dp"))
    back = 0
    for r in (3, 2, 1, 0):
        grad_pre[r] = (contract(low_two, w_downs[r], 1, 1) * ups[r][1].astype(F32)).astype(BF16)
        grad_b_up[r] = jnp.sum(grad_pre[r].astype(F32), 0, keepdims=True)
        grad_w_up[r] = contract(low_hidden, grad_pre[r], 0, 0).astype(BF16)
    for r in (3, 2, 1, 0):
        back = back + contract(grad_pre[r], w_ups[r], 1, 1)
    far = add_low(grad_w_up[2], swap(grad_w_up[3], "mp", 1))
    own = scatter_near(far, grad_w_up[0], grad_w_up[1])
    g_up = reduce_all(own, bits_of("dp"))
    grad_hidden = grad_two + back
    grad_one = norm_backward(grad_hidden, normed_one, inv_one, gain_one)
    low_one = grad_one.astype(BF16)
    whole = [
        jnp.sum(rows, 0, keepdims=True)
        for rows in (
            grad_one,
            grad_hidden * normed_one,
            grad_hidden,
            grad_two,
            grad_out * normed_two,
            grad_out,
        )
    ]

    grad_context = contract(w_out_all, low_one, 1, 1).astype(BF16)
    grad_w_out = contract(context, low_one, 1, 0).astype(BF16).reshape(4, part_cols, width)
    grad_context = grad_context.reshape(4, 1, part_heads, HD, frames)
    grad_attn, grad_qkv = [None] * 4, [None] * 4
    for r in (3, 2, 1, 0):
        qkv, ctx, inverse, probs = held[r]
        grads = attend_back(qkv, ctx, inverse, probs, grad_context[r])
        grads = grad_qkv[r] = grads.reshape(3 * part_cols, frames)
        grad_w = contract(grads, rows_in, 1, 0).astype(BF16)
        grad_attn[r] = jnp.concatenate([grad_w, grad_w_out[r]], 0)
    grad_x, sums = finish(grad_qkv, w_attn, grad_b_up + whole, grad_one)
    far = add_low(grad_attn[2], swap(grad_attn[3], "mp", 1))
    own = scatter_near(far, grad_attn[0], grad_attn[1])
    split = own.shape[0] // 2
    order = bits_of("dp")
    g_attn = jnp.concatenate(
        [reduce_all(own[:split], order), reduce_all(own[split:], order[1:] + order[:1])],
        0,
    ).astype(F32)
    sums = reduce_small(sums)
    grad_inputs = grad_x.reshape(inputs.shape)
    cols = part_cols
    return (
        output.astype(BF16).reshape(inputs.shape),
        grad_inputs,
        g_attn[:cols].T,
        sums[0, :cols],
        g_attn[cols : 2 * cols].T,
        g_attn[2 * cols : 3 * cols].T,
        sums[0, 2 * cols : 3 * cols],
        g_attn[3 * cols :],
        sums[2],
        sums[3],
        sums[4],
        g_up.astype(F32),
        sums[1],
        g_down.astype(F32),
        sums[5],
        sums[6],
        sums[7],
    )


def solution(mesh):
    clips = P(("dp", "mp"), None, None)
    placed = (
        clips,
        P("dp"),
        P(None, "mp"),
        P("mp"),
        P(None, "mp"),
        P(None, "mp"),
        P("mp"),
        P("mp", None),
        P(),
        P(),
        P(),
        P(None, "mp"),
        P("mp"),
        P("mp", None),
        P(),
        P(),
        P(),
        clips,
    )
    return jax.shard_map(
        per_device,
        mesh=mesh,
        in_specs=placed,
        out_specs=(clips, clips) + placed[2:17],
        check_vma=False,
    )
```

```python
from functools import partial

import jax
import jax.numpy as jnp
from jax import lax
from jax.experimental import pallas as pl
from jax.experimental.pallas import tpu as pltpu
from jax.sharding import PartitionSpec as P


HD = 64
EPS = 1e-05
F32 = jnp.float32
BF16 = jnp.bfloat16


def contract(left, right, left_dim, right_dim):
    return lax.dot_general(
        left, right, (((left_dim,), (right_dim,)), ((), ())), preferred_element_type=F32
    )


def attend_kernel(len_ref, q_ref, k_ref, v_ref, o_ref, inv_ref, p_ref):
    frames = q_ref.shape[-1]
    row = lax.broadcasted_iota(jnp.int32, (16, frames), 0)
    col = lax.broadcasted_iota(jnp.int32, (16, frames), 1)
    bias = jnp.where((row == 0) & (col >= len_ref[0]), -1e30, 0.0).astype(BF16)
    one = jnp.where(row == 0, 1.0, 0.0).astype(BF16)
    keys = jnp.concatenate([k_ref[...], bias], 0)
    scaled = (q_ref[...].astype(F32) * HD ** (-0.5)).astype(BF16)
    scores = contract(keys, jnp.concatenate([scaled, one], 0), 0, 0)
    probs = jnp.exp(scores - jnp.max(scores, 0, keepdims=True))
    inverse = 1.0 / jnp.sum(probs, 0, keepdims=True)
    low_probs = probs.astype(BF16)
    o_ref[...] = (contract(v_ref[...], low_probs, 1, 0) * inverse).astype(BF16)
    inv_ref[...] = inverse
    p_ref[...] = low_probs


def in_hbm(value):
    return pltpu.with_memory_space_constraint(value, pltpu.MemorySpace.HBM)


def attend(qkv, length):
    pieces, _, heads, _, frames = qkv.shape

    def part(which):
        return pl.BlockSpec(
            (None, None, None, HD, frames), lambda i: (i // heads, which, i % heads, 0, 0)
        )

    def out(rows):
        return pl.BlockSpec((None, None, rows, frames), lambda i: (i // heads, i % heads, 0, 0))

    shape = (pieces, heads)
    return pl.pallas_call(
        attend_kernel,
        grid=(pieces * heads,),
        out_shape=(
            jax.ShapeDtypeStruct(shape + (HD, frames), BF16),
            jax.ShapeDtypeStruct(shape + (1, frames), F32),
            pltpu.HBM(shape + (frames, frames), BF16),
        ),
        in_specs=[pl.BlockSpec(memory_space=pltpu.SMEM), part(0), part(1), part(2)],
        out_specs=(out(HD), out(1), out(frames)),
        compiler_params=pltpu.CompilerParams(vmem_limit_bytes=40 << 20),
        cost_estimate=pl.CostEstimate(
            flops=pieces * heads * frames * frames * 1024,
            bytes_accessed=pieces * heads * frames * frames * 2,
            transcendentals=0,
        ),
        name="attend",
    )(length, qkv, qkv, qkv)


def attend_back_kernel(q_ref, k_ref, v_ref, o_ref, inv_ref, p_ref, g_ref, out_ref):
    scaling = HD ** (-0.5)
    grad = g_ref[...].astype(F32) * inv_ref[...]
    row_dot = jnp.sum(grad * o_ref[...].astype(F32), 0, keepdims=True)
    low_grad = grad.astype(BF16)
    probs = p_ref[...]
    grad_probs = contract(v_ref[...], low_grad, 0, 0)
    grad_scores = probs * (grad_probs - row_dot).astype(BF16)
    out_ref[0] = (contract(k_ref[...], grad_scores, 1, 0) * scaling).astype(BF16)
    out_ref[1] = (contract(q_ref[...], grad_scores, 1, 1) * scaling).astype(BF16)
    out_ref[2] = contract(low_grad, probs, 1, 1).astype(BF16)


def attend_back(qkv, context, inverse, probs, grad_context):
    pieces, _, heads, _, frames = qkv.shape

    def part(which):
        return pl.BlockSpec(
            (None, None, None, HD, frames), lambda i: (i // heads, which, i % heads, 0, 0)
        )

    def one(rows):
        return pl.BlockSpec((None, None, rows, frames), lambda i: (i // heads, i % heads, 0, 0))

    return pl.pallas_call(
        attend_back_kernel,
        grid=(pieces * heads,),
        out_shape=jax.ShapeDtypeStruct(qkv.shape, BF16),
        in_specs=[part(0), part(1), part(2), one(HD), one(1), one(frames), one(HD)],
        out_specs=pl.BlockSpec(
            (None, 3, None, HD, frames), lambda i: (i // heads, 0, i % heads, 0, 0)
        ),
        compiler_params=pltpu.CompilerParams(vmem_limit_bytes=40 << 20),
        cost_estimate=pl.CostEstimate(
            flops=pieces * heads * frames * frames * 2048,
            bytes_accessed=pieces * heads * frames * frames * 2,
            transcendentals=0,
        ),
        name="attend_back",
    )(qkv, qkv, qkv, context, inverse, probs, grad_context)


def norm_forward(summed, gain_vec, shift_vec):
    centered = summed - jnp.mean(summed, -1, keepdims=True)
    inv_root = lax.rsqrt(jnp.mean(centered * centered, -1, keepdims=True) + EPS)
    normed = centered * inv_root
    return (normed * gain_vec + shift_vec, normed, inv_root)


def norm_backward(grad_in, normed, inv_root, gain_vec):
    scaled = grad_in * gain_vec
    return inv_root * (
        scaled
        - jnp.mean(scaled, -1, keepdims=True)
        - normed * jnp.mean(scaled * normed, -1, keepdims=True)
    )


def gelu_and_slope(pre):
    size = jnp.abs(pre)
    bell = jnp.exp(pre * pre * -0.5)
    t = 1.0 / (1.0 + (0.3275911 * 0.5**0.5) * size)
    series = t * (
        0.5 * 0.254829592
        + t
        * (
            0.5 * -0.284496736
            + t * (0.5 * 1.421413741 + t * (0.5 * -1.453152027 + t * (0.5 * 1.061405429)))
        )
    )
    tail = series * bell
    normal = jnp.where(pre >= 0, 1.0 - tail, tail)
    return pre * normal, normal + pre * bell * (2.0 * jnp.pi) ** -0.5


def ffn_kernel(count, last, *refs):
    refs = list(refs)

    def take(n):
        taken = refs[:n]
        del refs[:n]
        return taken

    (x_ref, base_ref), ups, biases, downs = take(2), take(count), take(count), take(count)
    if last:
        cot_ref, vec_ref = take(2)
    acts, slopes = take(count), take(count)
    total = base_ref[...]
    for r in range(count):
        pre = contract(x_ref[...], ups[r][...], 1, 0) + biases[r][...].astype(F32)
        act, slope = gelu_and_slope(pre)
        act = act.astype(BF16)
        acts[r][...] = act
        slopes[r][...] = slope.astype(BF16)
        total = total + contract(act, downs[r][...], 1, 0)
    if not last:
        refs[0][...] = total
        return
    out_ref, grad_ref, low_ref, sums_ref = refs
    gain = vec_ref[4:5]
    output, normed, inv_root = norm_forward(total + vec_ref[3:4], gain, vec_ref[5:6])
    out_ref[...] = output.astype(BF16)
    grad_out = cot_ref[...].astype(F32)
    grad = norm_backward(grad_out, normed, inv_root, gain)
    grad_ref[...] = grad
    low_ref[...] = grad.astype(BF16)

    @pl.when(pl.program_id(0) == 0)
    def _():
        sums_ref[...] = jnp.zeros(sums_ref.shape, F32)

    sums_ref[0:1] += jnp.sum(grad, 0, keepdims=True)
    sums_ref[1:2] += jnp.sum(grad_out * normed, 0, keepdims=True)
    sums_ref[2:3] += jnp.sum(grad_out, 0, keepdims=True)


def ffn(rows, base, ups, biases, downs, cotangent=None, vectors=None):
    frames, width = rows.shape
    units = ups[0].shape[1]
    count, last = len(ups), cotangent is not None
    tile = 256

    def tiled(cols):
        return pl.BlockSpec((tile, cols), lambda i: (i, 0))

    def fixed(shape):
        return pl.BlockSpec(shape, lambda i: (0, 0))

    def array(cols, dtype):
        return jax.ShapeDtypeStruct((frames, cols), dtype)

    out_shape = [array(units, BF16)] * (2 * count)
    out_specs = [tiled(units)] * (2 * count)
    args = [rows, base, *ups, *biases, *downs]
    in_specs = (
        [tiled(width)] * 2
        + [fixed((width, units))] * count
        + [fixed((1, units))] * count
        + [fixed((units, width))] * count
    )
    if last:
        args += [cotangent, vectors]
        in_specs += [tiled(width), fixed(vectors.shape)]
        out_shape += [array(width, BF16), array(width, F32), array(width, BF16)]
        out_shape.append(jax.ShapeDtypeStruct((8, width), F32))
        out_specs += [tiled(width)] * 3 + [fixed((8, width))]
    else:
        out_shape.append(array(width, F32))
        out_specs.append(tiled(width))
    result = pl.pallas_call(
        partial(ffn_kernel, count, last),
        grid=(frames // tile,),
        out_shape=out_shape,
        in_specs=in_specs,
        out_specs=out_specs,
        compiler_params=pltpu.CompilerParams(vmem_limit_bytes=40 << 20),
        cost_estimate=pl.CostEstimate(
            flops=4 * count * frames * width * units,
            bytes_accessed=frames * units * 8,
            transcendentals=0,
        ),
        name="ffn",
    )(*args)
    return result[:count], result[count : 2 * count], result[2 * count :]


def widen_kernel(*refs):
    refs[-1][...] = jnp.zeros(refs[-1].shape, F32)
    for k, ref in enumerate(refs[:-1]):
        refs[-1][k : k + 1, :] = ref[...].astype(F32).reshape(1, -1)


def widen(vectors):
    return pl.pallas_call(
        widen_kernel,
        out_shape=jax.ShapeDtypeStruct((8, vectors[0].shape[0]), F32),
        compiler_params=pltpu.CompilerParams(vmem_limit_bytes=4 << 20),
        cost_estimate=pl.CostEstimate(flops=1, bytes_accessed=1 << 20, transcendentals=0),
        name="widen",
    )(*vectors)


def swap(value, axis, bit):
    return lax.ppermute(value, axis, [(i, i ^ bit) for i in range(lax.axis_size(axis))])


def add_low(left, right):
    return (left.astype(F32) + right.astype(F32)).astype(left.dtype)


def scatter_near(far, near, near_other):
    near = add_low(near, swap(near_other, "mp", 1))
    return add_low(near, swap(far, "mp", 2))


def halve(value, bits):
    index = lax.axis_index("dp")
    for bit in bits:
        mine = (index // bit) % 2
        half = value.shape[0] // 2
        sent = lax.dynamic_slice_in_dim(value, (1 - mine) * half, half, 0)
        kept = lax.dynamic_slice_in_dim(value, mine * half, half, 0)
        value = add_low(kept, swap(sent, "dp", bit))
    return value


def double(value, bits):
    index = lax.axis_index("dp")
    for bit in bits:
        low_side = (index // bit) % 2 == 0
        other = swap(value, "dp", bit)
        value = jnp.concatenate(
            [jnp.where(low_side, value, other), jnp.where(low_side, other, value)], 0
        )
    return value


CHAINS = (
    ((1,), (2, 4), (4, 2, 1)),
    ((2,), (1, 4), (4, 1, 2)),
    ((2, 1), (4,), (4, 1, 2)),
    ((1,), (), (1,)),
)
CHAIN_STEPS = sum(len(halved) + len(doubled) for _, halved, doubled in CHAINS)


def bit_of(axis, bit):
    return lax.rem(lax.div(lax.axis_index(axis), bit), 2)


def partner(axis, bit):
    return {axis: lax.axis_index(axis) + bit * (1 - 2 * bit_of(axis, bit))}


def tail_kernel(groups, *refs):
    refs = list(refs)

    def take(n):
        taken = refs[:n]
        del refs[:n]
        return taken

    sources, (small_ref,) = take(len(CHAINS)), take(1)
    outs, (small_out,) = take(len(CHAINS)), take(1)
    fulls = take(len(CHAINS))
    halvings = sum(len(chain[1]) for chain in CHAINS)
    arrived, parts = take(halvings), take(halvings)
    group_got, group_buf, small_got, small_buf, send_sem, recv_sem = refs
    count = iter(range(CHAIN_STEPS + 5))
    started = []

    def send(src, dst, axis, bit):
        k = next(count)
        copy = pltpu.make_async_remote_copy(
            src_ref=src,
            dst_ref=dst,
            send_sem=send_sem.at[k],
            recv_sem=recv_sem.at[k],
            device_id=partner(axis, bit),
            device_id_type=pl.DeviceIdType.MESH,
        )
        copy.start()
        started.append(copy)
        return copy

    def chain(source, full, before, to_halve, to_double, got, summed):
        rows = full.shape[0]
        offset = 0
        for bit in before:
            rows = rows // 2
            offset = offset + bit_of("dp", bit) * rows
        for j, bit in enumerate(to_halve):
            rows = rows // 2
            mine = bit_of("dp", bit)
            away = pl.ds(pl.multiple_of((1 - mine) * rows, 16), rows)
            copy = send(source.at[away], got[j], "dp", bit)
            yield
            copy.wait_recv()
            kept = source[pl.ds(pl.multiple_of(mine * rows, 16), rows), :]
            summed[j][...] = add_low(kept, got[j][...])
            offset = offset + mine * rows
            source = summed[j]
        full[pl.ds(pl.multiple_of(offset, 16), rows), :] = source[...]
        for bit in to_double:
            place = full.at[pl.ds(pl.multiple_of(offset, 16), rows)]
            copy = send(place, place, "dp", bit)
            yield
            copy.wait_recv()
            offset = offset - bit_of("dp", bit) * rows
            rows = rows * 2

    def small():
        source = small_ref
        for j, bit in enumerate((1, 2)):
            copy = send(source, group_got.at[j], "mp", bit)
            yield
            copy.wait_recv()
            for r in range(groups):
                group_buf[j, r] = source[r] + group_got[j, r ^ bit]
            source = group_buf.at[j]
        total = source[0]
        row = lax.broadcasted_iota(jnp.int32, total.shape, 0)
        for r in range(1, groups):
            total = total + jnp.where(row < 2, 0.0, source[r])
        small_buf[0] = total
        for j, bit in enumerate((1, 2, 4)):
            copy = send(small_buf.at[j], small_got.at[j], "dp", bit)
            yield
            copy.wait_recv()
            small_buf[j + 1] = small_buf[j] + small_got[j]

    barrier = pltpu.get_barrier_semaphore()
    peers = [("dp", 1), ("dp", 2), ("dp", 4), ("mp", 1), ("mp", 2)]
    for axis, bit in peers:
        pl.semaphore_signal(
            barrier, inc=1, device_id=partner(axis, bit), device_id_type=pl.DeviceIdType.MESH
        )
    pl.semaphore_wait(barrier, len(peers))

    running = []
    used = 0
    for k, (before, to_halve, to_double) in enumerate(CHAINS):
        n = len(to_halve)
        pieces = (arrived[used : used + n], parts[used : used + n])
        running.append(chain(sources[k], fulls[k], before, to_halve, to_double, *pieces))
        used += n
    last = running.pop()
    running.append(small())
    for steps in running:
        next(steps)
    next(last)
    while running:
        running = [steps for steps in running if next(steps, last) is not last]
    next(last, None)
    for copy in started:
        copy.wait_send()
    for out, full in zip(outs, fulls):
        out[...] = full[...]
    small_out[...] = small_buf[3]


def tail(values, sums):
    groups, _, width = sums.shape
    vmem = pl.BlockSpec(memory_space=pltpu.VMEM)
    full_shapes, halved_shapes = [], []
    for value, (before, to_halve, _) in zip(values, CHAINS):
        rows = value.shape[0]
        full_shapes.append((rows << len(before), width))
        halved_shapes += [(rows >> (j + 1), width) for j in range(len(to_halve))]
    low = [pltpu.VMEM(shape, BF16) for shape in full_shapes]
    halved = [pltpu.VMEM(shape, BF16) for shape in halved_shapes]
    return pl.pallas_call(
        partial(tail_kernel, groups),
        out_shape=[jax.ShapeDtypeStruct(shape, BF16) for shape in full_shapes]
        + [jax.ShapeDtypeStruct(sums.shape[1:], F32)],
        in_specs=[vmem] * (len(values) + 1),
        out_specs=[vmem] * (len(values) + 1),
        scratch_shapes=low
        + halved
        + halved
        + [
            pltpu.VMEM((2,) + sums.shape, F32),
            pltpu.VMEM((2,) + sums.shape, F32),
            pltpu.VMEM((3,) + sums.shape[1:], F32),
            pltpu.VMEM((4,) + sums.shape[1:], F32),
            pltpu.SemaphoreType.DMA((CHAIN_STEPS + 5,)),
            pltpu.SemaphoreType.DMA((CHAIN_STEPS + 5,)),
        ],
        compiler_params=pltpu.CompilerParams(
            collective_id=1, has_side_effects=True, vmem_limit_bytes=32 << 20
        ),
        name="tail",
    )(*values, sums)


def finish_kernel(*refs):
    grads, weights, rows = refs[:4], refs[4:8], refs[8:15]
    sums_two_ref, base_ref, out_ref, sums_ref = refs[15:]
    cols = grads[0].shape[0]
    tile = grads[0].shape[1]

    @pl.when(pl.program_id(0) == 0)
    def _():
        sums_ref[...] = jnp.zeros(sums_ref.shape, F32)
        for r in range(4):
            sums_ref[r, 1:2, :] = rows[r][...]
        for k in range(3):
            sums_ref[0, 2 + k : 3 + k, :] = rows[4 + k][...]
            sums_ref[0, 5 + k : 6 + k, :] = sums_two_ref[k : k + 1]

    total = base_ref[...]
    ones = jnp.full((8, tile), 1.0, BF16)
    for r in range(4):
        piece = grads[r][...]
        total = total + contract(piece, weights[r][...], 0, 0)
        sums_ref[r, 0:1, :cols] += contract(ones, piece, 1, 1)[0:1]
    out_ref[...] = total.astype(BF16)


def finish(grads, weights, rows, base):
    frames, width = base.shape
    cols = grads[0].shape[0]
    tile = 256
    return pl.pallas_call(
        finish_kernel,
        grid=(frames // tile,),
        out_shape=(
            jax.ShapeDtypeStruct((frames, width), BF16),
            jax.ShapeDtypeStruct((4, 8, width), F32),
        ),
        in_specs=[pl.BlockSpec((cols, tile), lambda i: (0, i))] * 4
        + [pl.BlockSpec((cols, width), lambda i: (0, 0))] * 4
        + [pl.BlockSpec((1, width), lambda i: (0, 0))] * 7
        + [pl.BlockSpec((8, width), lambda i: (0, 0))]
        + [pl.BlockSpec((tile, width), lambda i: (i, 0))],
        out_specs=(
            pl.BlockSpec((tile, width), lambda i: (i, 0)),
            pl.BlockSpec((4, 8, width), lambda i: (0, 0, 0)),
        ),
        compiler_params=pltpu.CompilerParams(vmem_limit_bytes=40 << 20),
        cost_estimate=pl.CostEstimate(
            flops=8 * frames * width * cols, bytes_accessed=frames * width * 12, transcendentals=0
        ),
        name="finish",
    )(*grads, *weights, *rows, base)


def per_device(
    inputs,
    lengths,
    w_query,
    b_query,
    w_key,
    w_value,
    b_value,
    w_out,
    b_out,
    gain_one,
    shift_one,
    w_up,
    b_up,
    w_down,
    b_down,
    gain_two,
    shift_two,
    cotangent,
):
    own_clips, frames, width = inputs.shape
    part_cols = w_query.shape[1]
    part_heads = part_cols // HD
    rows_in = inputs.reshape(own_clips * frames, width)
    length = lax.dynamic_slice_in_dim(lengths, lax.axis_index("mp") * own_clips, own_clips, 0)

    def gather(own):
        far = swap(own, "mp", 2)
        return [own, swap(own, "mp", 1), far, swap(far, "mp", 1)]

    w_attn = gather(jnp.concatenate([w_query.T, w_key.T, w_value.T], 0))
    biases = gather(
        jnp.concatenate([b_query, jnp.zeros_like(b_query), b_value, b_up], 0).reshape(1, -1)
    )
    w_outs = gather(w_out)

    def gather_halves(own):
        half = own.shape[0] // 2
        side = lax.axis_index("dp") % 2
        got = swap(lax.dynamic_slice_in_dim(own, side * half, half, 0), "mp", 2)
        other = swap(got, "dp", 1)
        low = side == 0
        far = jnp.concatenate([jnp.where(low, got, other), jnp.where(low, other, got)], 0)
        return [own, swap(own, "mp", 1), far, swap(far, "mp", 1)]

    w_ups = gather_halves(w_up)
    w_downs = gather_halves(w_down)
    vectors = widen([b_out, gain_one, shift_one, b_down, gain_two, shift_two])
    b_out, gain_one, shift_one = [vectors[k : k + 1] for k in range(3)]

    held = []
    for r in range(4):
        bias = biases[r][0, : 3 * part_cols].astype(F32)[:, None]
        qkv = (contract(w_attn[r], rows_in, 1, 1) + bias).astype(BF16)
        qkv = qkv.reshape(1, 3, part_heads, HD, frames)
        ctx, inverse, probs = attend(qkv, length)
        held.append((qkv, ctx, inverse, in_hbm(probs)))
    context = jnp.concatenate([h[1].reshape(part_cols, frames) for h in held], 0)
    w_out_all = jnp.concatenate(w_outs, 0)
    mixed = contract(context, w_out_all, 0, 0)
    first_sum = rows_in.astype(F32) + mixed + b_out
    hidden, normed_one, inv_one = norm_forward(first_sum, gain_one, shift_one)
    low_hidden = hidden.astype(BF16)

    up_bias = [biases[r][:, 3 * part_cols :] for r in range(4)]
    acts, slopes, (total,) = ffn(low_hidden, hidden, w_ups[:2], up_bias[:2], w_downs[:2])
    more = ffn(low_hidden, total, w_ups[2:3], up_bias[2:3], w_downs[2:3])
    acts, slopes, (total,) = acts + more[0], slopes + more[1], more[2]
    grad_out = cotangent.reshape(own_clips * frames, width)
    more = ffn(low_hidden, total, w_ups[3:], up_bias[3:], w_downs[3:], grad_out, vectors)
    acts, slopes = acts + more[0], slopes + more[1]
    output, grad_two, low_two, sums_two = more[2]

    grad_w_down, grad_w_up, grad_b_up = [None] * 4, [None] * 4, [None] * 4
    grad_pre = [None] * 4
    for r in (3, 2, 1, 0):
        grad_w_down[r] = contract(acts[r], low_two, 0, 0).astype(BF16)
    far = add_low(grad_w_down[2], swap(grad_w_down[3], "mp", 1))
    own = scatter_near(far, grad_w_down[0], grad_w_down[1])
    d_last = double(halve(own, (1, 2, 4)), (4, 2))
    back = 0
    for r in (3, 2, 1, 0):
        grad_pre[r] = (contract(low_two, w_downs[r], 1, 1) * slopes[r].astype(F32)).astype(BF16)
        grad_b_up[r] = jnp.sum(grad_pre[r].astype(F32), 0, keepdims=True)
        grad_w_up[r] = contract(low_hidden, grad_pre[r], 0, 0).astype(BF16)
    for r in (3, 2, 1, 0):
        back = back + contract(grad_pre[r], w_ups[r], 1, 1)
    far = add_low(grad_w_up[2], swap(grad_w_up[3], "mp", 1))
    own = scatter_near(far, grad_w_up[0], grad_w_up[1])
    u_last = halve(own, (2, 1))
    grad_hidden = grad_two + back
    grad_one = norm_backward(grad_hidden, normed_one, inv_one, gain_one)
    low_one = grad_one.astype(BF16)
    whole = [
        jnp.sum(rows, 0, keepdims=True)
        for rows in (
            grad_one,
            grad_hidden * normed_one,
            grad_hidden,
        )
    ]

    grad_context = contract(w_out_all, low_one, 1, 1).astype(BF16)
    grad_w_out = contract(context, low_one, 1, 0).astype(BF16).reshape(4, part_cols, width)
    grad_context = grad_context.reshape(4, 1, part_heads, HD, frames)
    grad_attn, grad_qkv = [None] * 4, [None] * 4
    for r in (3, 2, 1, 0):
        qkv, ctx, inverse, probs = held[r]
        grads = attend_back(qkv, ctx, inverse, probs, grad_context[r])
        grads = grad_qkv[r] = grads.reshape(3 * part_cols, frames)
        grad_w = contract(grads, rows_in, 1, 0).astype(BF16)
        grad_attn[r] = jnp.concatenate([grad_w, grad_w_out[r]], 0)
    grad_x, sums = finish(grad_qkv, w_attn, grad_b_up + whole + [sums_two], grad_one)
    far = add_low(grad_attn[2], swap(grad_attn[3], "mp", 1))
    own = scatter_near(far, grad_attn[0], grad_attn[1])
    split = own.shape[0] // 2
    a_last, b_last = halve(own[:split], (1,)), halve(own[split:], (2,))
    g_first, g_second, g_up, g_down, sums = tail([a_last, b_last, u_last, d_last], sums)
    g_attn = jnp.concatenate([g_first, g_second], 0).astype(F32)
    grad_inputs = grad_x.reshape(inputs.shape)
    cols = part_cols
    return (
        output.reshape(inputs.shape),
        grad_inputs,
        g_attn[:cols].T,
        sums[0, :cols],
        g_attn[cols : 2 * cols].T,
        g_attn[2 * cols : 3 * cols].T,
        sums[0, 2 * cols : 3 * cols],
        g_attn[3 * cols :],
        sums[2],
        sums[3],
        sums[4],
        g_up.astype(F32),
        sums[1],
        g_down.astype(F32),
        sums[5],
        sums[6],
        sums[7],
    )


def solution(mesh):
    clips = P(("dp", "mp"), None, None)
    placed = (
        clips,
        P("dp"),
        P(None, "mp"),
        P("mp"),
        P(None, "mp"),
        P(None, "mp"),
        P("mp"),
        P("mp", None),
        P(),
        P(),
        P(),
        P(None, "mp"),
        P("mp"),
        P("mp", None),
        P(),
        P(),
        P(),
        clips,
    )
    return jax.shard_map(
        per_device,
        mesh=mesh,
        in_specs=placed,
        out_specs=(clips, clips) + placed[2:17],
        check_vma=False,
    )
```

```python
from functools import partial

import jax
import jax.numpy as jnp
from jax import lax
from jax.experimental import pallas as pl
from jax.experimental.pallas import tpu as pltpu
from jax.sharding import PartitionSpec as P


HD = 64
EPS = 1e-05
F32 = jnp.float32
BF16 = jnp.bfloat16


def contract(left, right, left_dim, right_dim):
    return lax.dot_general(
        left, right, (((left_dim,), (right_dim,)), ((), ())), preferred_element_type=F32
    )


def attend_kernel(len_ref, q_ref, k_ref, v_ref, o_ref, inv_ref, p_ref):
    frames = q_ref.shape[-1]
    row = lax.broadcasted_iota(jnp.int32, (16, frames), 0)
    col = lax.broadcasted_iota(jnp.int32, (16, frames), 1)
    bias = jnp.where((row == 0) & (col >= len_ref[0]), -1e30, 0.0).astype(BF16)
    one = jnp.where(row == 0, 1.0, 0.0).astype(BF16)
    keys = jnp.concatenate([k_ref[...], bias], 0)
    scaled = (q_ref[...].astype(F32) * HD ** (-0.5)).astype(BF16)
    scores = contract(keys, jnp.concatenate([scaled, one], 0), 0, 0)
    probs = jnp.exp(scores - jnp.max(scores, 0, keepdims=True))
    inverse = 1.0 / jnp.sum(probs, 0, keepdims=True)
    low_probs = probs.astype(BF16)
    o_ref[...] = (contract(v_ref[...], low_probs, 1, 0) * inverse).astype(BF16)
    inv_ref[...] = inverse
    p_ref[...] = low_probs


def in_hbm(value):
    return pltpu.with_memory_space_constraint(value, pltpu.MemorySpace.HBM)


def attend(qkv, length):
    pieces, _, heads, _, frames = qkv.shape

    def part(which):
        return pl.BlockSpec(
            (None, None, None, HD, frames), lambda i: (i // heads, which, i % heads, 0, 0)
        )

    def out(rows):
        return pl.BlockSpec((None, None, rows, frames), lambda i: (i // heads, i % heads, 0, 0))

    shape = (pieces, heads)
    return pl.pallas_call(
        attend_kernel,
        grid=(pieces * heads,),
        out_shape=(
            jax.ShapeDtypeStruct(shape + (HD, frames), BF16),
            jax.ShapeDtypeStruct(shape + (1, frames), F32),
            pltpu.HBM(shape + (frames, frames), BF16),
        ),
        in_specs=[pl.BlockSpec(memory_space=pltpu.SMEM), part(0), part(1), part(2)],
        out_specs=(out(HD), out(1), out(frames)),
        compiler_params=pltpu.CompilerParams(vmem_limit_bytes=40 << 20),
        cost_estimate=pl.CostEstimate(
            flops=pieces * heads * frames * frames * 1024,
            bytes_accessed=pieces * heads * frames * frames * 2,
            transcendentals=0,
        ),
        name="attend",
    )(length, qkv, qkv, qkv)


def norm_forward(summed, gain_vec, shift_vec):
    centered = summed - jnp.mean(summed, -1, keepdims=True)
    inv_root = lax.rsqrt(jnp.mean(centered * centered, -1, keepdims=True) + EPS)
    normed = centered * inv_root
    return (normed * gain_vec + shift_vec, normed, inv_root)


def norm_backward(grad_in, normed, inv_root, gain_vec):
    scaled = grad_in * gain_vec
    return inv_root * (
        scaled
        - jnp.mean(scaled, -1, keepdims=True)
        - normed * jnp.mean(scaled * normed, -1, keepdims=True)
    )


def gelu_and_slope(pre):
    size = jnp.abs(pre)
    bell = jnp.exp(pre * pre * -0.5)
    t = 1.0 / (1.0 + (0.3275911 * 0.5**0.5) * size)
    series = t * (
        0.5 * 0.254829592
        + t
        * (
            0.5 * -0.284496736
            + t * (0.5 * 1.421413741 + t * (0.5 * -1.453152027 + t * (0.5 * 1.061405429)))
        )
    )
    tail = series * bell
    normal = jnp.where(pre >= 0, 1.0 - tail, tail)
    return pre * normal, normal + pre * bell * (2.0 * jnp.pi) ** -0.5


def ffn_kernel(count, last, *refs):
    refs = list(refs)

    def take(n):
        taken = refs[:n]
        del refs[:n]
        return taken

    (x_ref, base_ref), ups, biases, downs = take(2), take(count), take(count), take(count)
    if last:
        cot_ref, vec_ref = take(2)
    acts, slopes = take(count), take(count)
    total = base_ref[...]
    for r in range(count):
        pre = contract(x_ref[...], ups[r][...], 1, 0) + biases[r][...].astype(F32)
        act, slope = gelu_and_slope(pre)
        act = act.astype(BF16)
        acts[r][...] = act
        slopes[r][...] = slope.astype(BF16)
        total = total + contract(act, downs[r][...], 1, 0)
    if not last:
        refs[0][...] = total
        return
    out_ref, grad_ref, low_ref, sums_ref = refs
    gain = vec_ref[4:5]
    output, normed, inv_root = norm_forward(total + vec_ref[3:4], gain, vec_ref[5:6])
    out_ref[...] = output.astype(BF16)
    grad_out = cot_ref[...].astype(F32)
    grad = norm_backward(grad_out, normed, inv_root, gain)
    grad_ref[...] = grad
    low_ref[...] = grad.astype(BF16)

    @pl.when(pl.program_id(0) == 0)
    def _():
        sums_ref[...] = jnp.zeros(sums_ref.shape, F32)

    sums_ref[0:1] += jnp.sum(grad, 0, keepdims=True)
    sums_ref[1:2] += jnp.sum(grad_out * normed, 0, keepdims=True)
    sums_ref[2:3] += jnp.sum(grad_out, 0, keepdims=True)


def ffn(rows, base, ups, biases, downs, cotangent=None, vectors=None):
    frames, width = rows.shape
    units = ups[0].shape[1]
    count, last = len(ups), cotangent is not None
    tile = 256

    def tiled(cols):
        return pl.BlockSpec((tile, cols), lambda i: (i, 0))

    def fixed(shape):
        return pl.BlockSpec(shape, lambda i: (0, 0))

    def array(cols, dtype):
        return jax.ShapeDtypeStruct((frames, cols), dtype)

    out_shape = [array(units, BF16)] * (2 * count)
    out_specs = [tiled(units)] * (2 * count)
    args = [rows, base, *ups, *biases, *downs]
    in_specs = (
        [tiled(width)] * 2
        + [fixed((width, units))] * count
        + [fixed((1, units))] * count
        + [fixed((units, width))] * count
    )
    if last:
        args += [cotangent, vectors]
        in_specs += [tiled(width), fixed(vectors.shape)]
        out_shape += [array(width, BF16), array(width, F32), array(width, BF16)]
        out_shape.append(jax.ShapeDtypeStruct((8, width), F32))
        out_specs += [tiled(width)] * 3 + [fixed((8, width))]
    else:
        out_shape.append(array(width, F32))
        out_specs.append(tiled(width))
    result = pl.pallas_call(
        partial(ffn_kernel, count, last),
        grid=(frames // tile,),
        out_shape=out_shape,
        in_specs=in_specs,
        out_specs=out_specs,
        compiler_params=pltpu.CompilerParams(vmem_limit_bytes=40 << 20),
        cost_estimate=pl.CostEstimate(
            flops=4 * count * frames * width * units,
            bytes_accessed=frames * units * 8,
            transcendentals=0,
        ),
        name="ffn",
    )(*args)
    return result[:count], result[count : 2 * count], result[2 * count :]


def widen_kernel(*refs):
    refs[-1][...] = jnp.zeros(refs[-1].shape, F32)
    for k, ref in enumerate(refs[:-1]):
        refs[-1][k : k + 1, :] = ref[...].astype(F32).reshape(1, -1)


def widen(vectors):
    return pl.pallas_call(
        widen_kernel,
        out_shape=jax.ShapeDtypeStruct((8, vectors[0].shape[0]), F32),
        compiler_params=pltpu.CompilerParams(vmem_limit_bytes=4 << 20),
        cost_estimate=pl.CostEstimate(flops=1, bytes_accessed=1 << 20, transcendentals=0),
        name="widen",
    )(*vectors)


def swap(value, axis, bit):
    return lax.ppermute(value, axis, [(i, i ^ bit) for i in range(lax.axis_size(axis))])


def bits_of(axis):
    return [1 << b for b in range(lax.axis_size(axis).bit_length() - 1)]


def add_low(left, right):
    return (left.astype(F32) + right.astype(F32)).astype(left.dtype)


def sum_near(near, near_other):
    return add_low(near, swap(near_other, "mp", 1))


def sum_far(near, far):
    return add_low(near, swap(far, "mp", 2))


D_ORDERS = ((1, 2, 4), (2, 1, 4), (4, 1, 2))
U_ORDERS = ((1, 2, 4), (1, 4, 2), (2, 1, 4))
A_ORDERS = ((1, 2, 4), (1, 4, 2), (2, 1, 4))

LATE = 99
FAR_EVENTS = (
    (3, 0, 0), (4, 1, 0), (4, 2, 0), (5, 0, 1), (LATE, 1, 1), (LATE, 2, 1), (LATE, 0, 2),
    (LATE, 1, 2), (LATE, 2, 2),
)
NEAR_EVENTS = (
    (3, 0, 0), (3, 1, 0), (3, 2, 0), (4, 5, 0), (4, 3, 0), (4, 4, 0), (5, 0, 1), (LATE, 1, 1),
    (LATE, 2, 1), (LATE, 3, 1), (LATE, 4, 1), (LATE, 5, 1), (LATE, 0, 2), (LATE, 4, 2),
    (LATE, 3, 2), (LATE, 5, 2), (LATE, 1, 2), (LATE, 2, 2),
)
END_EVENTS = (
    (3, 0), (4, 0), (5, 0), (0, 0), (1, 0), (5, 1), (2, 0), (3, 1), (4, 1), (2, 1), (0, 1), (1, 1),
    (2, 2), (0, 2), (1, 2), (3, 2), (4, 2), (5, 2), (2, 3), (1, 3), (0, 3), (2, 4), (1, 4), (0, 4),
    (2, 5), (1, 5), (0, 5),
)


def reduce_rest(value):
    for bit in bits_of("dp")[3:]:
        value = add_low(value, swap(value, "dp", bit))
    return value


def bit_of(axis, bit):
    return lax.rem(lax.div(lax.axis_index(axis), bit), 2)


def partner(axis, bit):
    return {axis: lax.axis_index(axis) + bit * (1 - 2 * bit_of(axis, bit))}


def rows_at(start, size):
    return pl.ds(pl.multiple_of(start, 16), size)


def greet(peers):
    barrier = pltpu.get_barrier_semaphore()
    for axis, bit in peers:
        pl.semaphore_signal(
            barrier, inc=1, device_id=partner(axis, bit), device_id_type=pl.DeviceIdType.MESH
        )
    pl.semaphore_wait(barrier, len(peers))


def remote(src, dst, send_sem, recv_sem, axis, bit):
    return pltpu.make_async_remote_copy(
        src_ref=src,
        dst_ref=dst,
        send_sem=send_sem,
        recv_sem=recv_sem,
        device_id=partner(axis, bit),
        device_id_type=pl.DeviceIdType.MESH,
    )


class Chain:
    def __init__(self, rows, order, halving, doubling, source, source_base, full, full_base):
        self.rows, self.order = rows, order
        self.halves = order if halving else ()
        self.doubles = order[::-1] if doubling else ()
        self.before = () if halving else order
        self.source, self.source_base = source, source_base
        self.full, self.full_base = full, full_base
        self.stages = len(self.halves) + len(self.doubles)

    def scratch(self):
        sizes = [self.rows >> (j + 1) for j in range(len(self.halves))]
        return sizes + sizes

    def bind(self, buffers, sems):
        n = len(self.halves)
        self.got, self.summed, self.sems = buffers[:n], buffers[n:], sems

    def place(self, stage):
        size, offset = self.rows, 0
        for bit in self.before + self.halves[:stage]:
            size = size // 2
            offset = offset + bit_of("dp", bit) * size
        for bit in self.doubles[: max(0, stage - len(self.halves))]:
            offset = offset - bit_of("dp", bit) * size
            size = size * 2
        return offset, size

    def held(self, stage):
        return (self.summed[stage - 1], 0) if stage else (self.source, self.source_base)

    def copy(self, stage):
        send_sem, recv_sem = self.sems[stage]
        offset, size = self.place(stage)
        if stage < len(self.halves):
            bit = self.halves[stage]
            ref, base = self.held(stage)
            away = rows_at(base + (1 - bit_of("dp", bit)) * (size // 2), size // 2)
            return remote(ref.at[away], self.got[stage], send_sem, recv_sem, "dp", bit)
        place = self.full.at[rows_at(self.full_base + offset, size)]
        bit = self.doubles[stage - len(self.halves)]
        return remote(place, place, send_sem, recv_sem, "dp", bit)

    def start(self, stage):
        n = len(self.halves)
        if stage == n:
            offset, size = self.place(stage)
            ref, base = self.held(n)
            self.full[rows_at(self.full_base + offset, size), :] = ref[base : base + size, :]
        self.copy(stage).start()

    def finish(self, stage):
        self.copy(stage).wait_recv()
        if stage < len(self.halves):
            size = self.place(stage)[1] // 2
            ref, base = self.held(stage)
            mine = bit_of("dp", self.halves[stage])
            kept = ref[rows_at(base + mine * size, size), :]
            self.summed[stage][...] = add_low(kept, self.got[stage][...])

    def step(self, stage):
        if 0 < stage <= self.stages:
            self.finish(stage - 1)
        if stage < self.stages:
            self.start(stage)


def split_rows(rows):
    return (rows // 3,) * 3


def chains_of(rows, halving, doubling, orders, source=None, full=None):
    made, source_base, full_base = [], 0, 0
    for part, order in zip(split_rows(rows), orders):
        made.append(
            Chain(part, order, halving, doubling, source, source_base, full, full_base)
        )
        source_base += part if halving else part >> len(order)
        full_base += part
    return made


class Reductions:
    def __init__(self, plans):
        self.plans = plans

    def out_rows(self):
        return [rows if doubling else rows >> 3 for rows, _, doubling, _ in self.plans]

    def scratch(self, width):
        shapes = []
        for rows, halving, doubling, orders in self.plans:
            if doubling:
                shapes.append(pltpu.VMEM((rows, width), BF16))
            for chain in chains_of(rows, halving, doubling, orders):
                shapes += [pltpu.VMEM((n, width), BF16) for n in chain.scratch()]
        return shapes

    def count(self):
        return sum(c.stages for plan in self.plans for c in chains_of(*plan))

    def bind(self, sources, refs, send_sem, recv_sem):
        self.groups, self.chains, k = [], [], 0
        for (rows, halving, doubling, orders), source in zip(self.plans, sources):
            full = refs.pop(0) if doubling else None
            made = chains_of(rows, halving, doubling, orders, source, full)
            for chain in made:
                n = len(chain.scratch())
                sems = [(send_sem.at[k + j], recv_sem.at[k + j]) for j in range(chain.stages)]
                k += chain.stages
                chain.bind(refs[:n], sems)
                del refs[:n]
            self.groups.append((full, made))
            self.chains += made

    def start(self):
        for chain in self.chains:
            chain.step(0)

    def arrive(self, events):
        for k, stage in events:
            self.chains[k].step(stage + 1)

    def close(self, outs):
        for chain in self.chains:
            for stage in range(chain.stages):
                chain.copy(stage).wait_send()
        for out, (full, made) in zip(outs, self.groups):
            if full is not None:
                out[...] = full[...]
                continue
            base = 0
            for chain in made:
                size = chain.rows >> len(chain.halves)
                out[base : base + size, :] = chain.summed[-1][...]
                base += size


def attend_back_kernel(plans, events, q_ref, k_ref, v_ref, o_ref, inv_ref, p_ref, g_ref, *refs):
    refs = list(refs)
    n = len(plans)
    sources, out_ref, outs = refs[:n], refs[n], refs[n + 1 : 2 * n + 1]
    send_sem, recv_sem = refs[-2:]
    reductions = Reductions(plans)
    reductions.bind(sources, refs[2 * n + 1 : -2], send_sem, recv_sem)
    step, steps = pl.program_id(0), pl.num_programs(0)

    @pl.when(step == 0)
    def _():
        greet([("dp", 1), ("dp", 2), ("dp", 4)])
        reductions.start()

    for slot in sorted({e[0] for e in events} - {LATE}):

        @pl.when(step == slot)
        def _(slot=slot):
            reductions.arrive([e[1:] for e in events if e[0] == slot])

    scaling = HD ** (-0.5)
    grad = g_ref[...].astype(F32) * inv_ref[...]
    row_dot = jnp.sum(grad * o_ref[...].astype(F32), 0, keepdims=True)
    low_grad = grad.astype(BF16)
    probs = p_ref[...]
    grad_probs = contract(v_ref[...], low_grad, 0, 0)
    grad_scores = probs * (grad_probs - row_dot).astype(BF16)
    out_ref[0] = (contract(k_ref[...], grad_scores, 1, 0) * scaling).astype(BF16)
    out_ref[1] = (contract(q_ref[...], grad_scores, 1, 1) * scaling).astype(BF16)
    out_ref[2] = contract(low_grad, probs, 1, 1).astype(BF16)

    @pl.when(step == steps - 1)
    def _():
        reductions.arrive([e[1:] for e in events if e[0] == LATE])
        reductions.close(outs)


def attend_back(qkv, context, inverse, probs, grad_context, plans, events, values, collective_id):
    pieces, _, heads, _, frames = qkv.shape
    assert max(e[0] for e in events if e[0] != LATE) < pieces * heads
    width = values[0].shape[1]

    def part(which):
        return pl.BlockSpec(
            (None, None, None, HD, frames), lambda i: (i // heads, which, i % heads, 0, 0)
        )

    def one(rows):
        return pl.BlockSpec((None, None, rows, frames), lambda i: (i // heads, i % heads, 0, 0))

    reductions = Reductions(plans)
    vmem = pl.BlockSpec(memory_space=pltpu.VMEM)
    sems = pltpu.SemaphoreType.DMA((reductions.count(),))
    return pl.pallas_call(
        partial(attend_back_kernel, plans, events),
        grid=(pieces * heads,),
        out_shape=[jax.ShapeDtypeStruct(qkv.shape, BF16)]
        + [jax.ShapeDtypeStruct((rows, width), BF16) for rows in reductions.out_rows()],
        in_specs=[part(0), part(1), part(2), one(HD), one(1), one(frames), one(HD)]
        + [vmem] * len(plans),
        out_specs=[
            pl.BlockSpec((None, 3, None, HD, frames), lambda i: (i // heads, 0, i % heads, 0, 0))
        ]
        + [vmem] * len(plans),
        scratch_shapes=reductions.scratch(width) + [sems, sems],
        compiler_params=pltpu.CompilerParams(
            vmem_limit_bytes=44 << 20, collective_id=collective_id, has_side_effects=True
        ),
        cost_estimate=pl.CostEstimate(
            flops=pieces * heads * frames * frames * 2048,
            bytes_accessed=pieces * heads * frames * frames * 2,
            transcendentals=0,
        ),
        name="attend_back",
    )(qkv, qkv, qkv, context, inverse, probs, grad_context, *values)


def finish_kernel(plans, *refs):
    refs = list(refs)

    def take(n):
        taken = refs[:n]
        del refs[:n]
        return taken

    n = len(plans)
    sources, grads, weights, rows = take(n), take(2), take(2), take(7)
    sums_two_ref, base_ref = take(2)
    outs, (out_ref, small_out) = take(n), take(2)
    send_sem, recv_sem = refs.pop(), None
    recv_sem, send_sem = send_sem, refs.pop()
    group_buf, group_got, small_buf, small_got = [refs.pop() for _ in range(4)]
    reductions = Reductions(plans)
    reductions.bind(sources, refs, send_sem, recv_sem)
    first_sem = reductions.count()
    part = grads[0].shape[0] // 2
    frames = base_ref.shape[0]
    tiles = 4
    tile = frames // tiles

    greet([("dp", 1), ("dp", 2), ("dp", 4), ("mp", 1), ("mp", 2)])
    reductions.start()

    group_buf[0] = jnp.zeros(group_buf.shape[1:], F32)
    for r in range(4):
        group_buf[0, r, 1:2, :] = rows[r][...]
    for k in range(3):
        group_buf[0, 0, 2 + k : 3 + k, :] = rows[4 + k][...]
        group_buf[0, 0, 5 + k : 6 + k, :] = sums_two_ref[k : k + 1]
    ones = jnp.full((8, tile), 1.0, BF16)

    def input_tile(t):
        place = slice(t * tile, (t + 1) * tile)
        total = base_ref[place, :]
        for k in range(2):
            piece = grads[k][:, place]
            total = total + contract(piece, weights[k][...], 0, 0)
            sums = contract(ones, piece, 1, 1)
            for r in range(2):
                mine = sums[0:1, r * part : (r + 1) * part]
                group_buf[0, 2 * k + r, 0:1, :part] += mine
        out_ref[place, :] = total.astype(BF16)

    small_steps = (("mp", 1), ("mp", 2), ("dp", 1), ("dp", 2), ("dp", 4))

    def small_copy(j):
        axis, bit = small_steps[j]
        pair = (group_buf, group_got) if axis == "mp" else (small_buf, small_got)
        index = j if axis == "mp" else j - 2
        sems = (send_sem.at[first_sem + j], recv_sem.at[first_sem + j])
        return remote(pair[0].at[index], pair[1].at[index], *sems, axis, bit)

    def small_finish(j):
        small_copy(j).wait_recv()
        if j >= 2:
            small_buf[j - 1] = small_buf[j - 2] + small_got[j - 2]
            return
        bit = small_steps[j][1]
        groups = [group_buf[j, r] + group_got[j, r ^ bit] for r in range(4)]
        for r in range(4):
            group_buf[j + 1, r] = groups[r]
        if j == 1:
            row = lax.broadcasted_iota(jnp.int32, groups[0].shape, 0)
            small_buf[0] = groups[0] + jnp.where(row < 2, 0.0, groups[1] + groups[2] + groups[3])

    input_tile(0)
    input_tile(1)
    reductions.arrive(END_EVENTS[:3])
    input_tile(2)
    reductions.arrive(END_EVENTS[3:5])
    input_tile(3)
    small_copy(0).start()
    for j in range(5):
        reductions.arrive(END_EVENTS[5 + 3 * j : 8 + 3 * j])
        small_finish(j)
        if j + 1 < 5:
            small_copy(j + 1).start()
    reductions.arrive(END_EVENTS[20:])
    for j in range(5):
        small_copy(j).wait_send()
    reductions.close(outs)
    small_out[...] = small_buf[3]


def finish(plans, values, grads, weights, rows, base):
    frames, width = base.shape
    reductions = Reductions(plans)
    vmem = pl.BlockSpec(memory_space=pltpu.VMEM)
    args = [*values, *grads, *weights, *rows, base]
    sems = pltpu.SemaphoreType.DMA((reductions.count() + 5,))
    return pl.pallas_call(
        partial(finish_kernel, plans),
        out_shape=[jax.ShapeDtypeStruct((n, width), BF16) for n in reductions.out_rows()]
        + [jax.ShapeDtypeStruct((frames, width), BF16), jax.ShapeDtypeStruct((8, width), F32)],
        in_specs=[vmem] * len(args),
        out_specs=[vmem] * (len(plans) + 2),
        scratch_shapes=reductions.scratch(width)
        + [
            pltpu.VMEM((3, 8, width), F32),
            pltpu.VMEM((4, 8, width), F32),
            pltpu.VMEM((2, 4, 8, width), F32),
            pltpu.VMEM((3, 4, 8, width), F32),
            sems,
            sems,
        ],
        compiler_params=pltpu.CompilerParams(
            collective_id=1, has_side_effects=True, vmem_limit_bytes=48 << 20
        ),
        name="finish",
    )(*args)


def per_device(
    inputs,
    lengths,
    w_query,
    b_query,
    w_key,
    w_value,
    b_value,
    w_out,
    b_out,
    gain_one,
    shift_one,
    w_up,
    b_up,
    w_down,
    b_down,
    gain_two,
    shift_two,
    cotangent,
):
    own_clips, frames, width = inputs.shape
    assert lax.axis_size("dp") >= 8 and lax.axis_size("mp") == 4
    part_cols = w_query.shape[1]
    part_heads = part_cols // HD
    rows_in = inputs.reshape(own_clips * frames, width)
    length = lax.dynamic_slice_in_dim(lengths, lax.axis_index("mp") * own_clips, own_clips, 0)

    def gather(own):
        far = swap(own, "mp", 2)
        return [own, swap(own, "mp", 1), far, swap(far, "mp", 1)]

    w_attn = gather(jnp.concatenate([w_query.T, w_key.T, w_value.T], 0))
    biases = gather(
        jnp.concatenate([b_query, jnp.zeros_like(b_query), b_value, b_up], 0).reshape(1, -1)
    )
    w_outs = gather(w_out)

    def gather_halves(own):
        half = own.shape[0] // 2
        side = lax.axis_index("dp") % 2
        got = swap(lax.dynamic_slice_in_dim(own, side * half, half, 0), "mp", 2)
        other = swap(got, "dp", 1)
        low = side == 0
        far = jnp.concatenate([jnp.where(low, got, other), jnp.where(low, other, got)], 0)
        return [own, swap(own, "mp", 1), far, swap(far, "mp", 1)]

    w_ups = gather_halves(w_up)
    w_downs = gather_halves(w_down)
    vectors = widen([b_out, gain_one, shift_one, b_down, gain_two, shift_two])
    b_out, gain_one, shift_one = [vectors[k : k + 1] for k in range(3)]

    held, w_pairs = [], []
    for k in range(2):
        pair = range(2 * k, 2 * k + 2)
        weight = jnp.concatenate([w_attn[r] for r in pair], 0)
        bias = jnp.concatenate([biases[r][0, : 3 * part_cols] for r in pair], 0)
        qkv = (contract(weight, rows_in, 1, 1) + bias.astype(F32)[:, None]).astype(BF16)
        qkv = qkv.reshape(2, 3, part_heads, HD, frames)
        ctx, inverse, probs = attend(qkv, length)
        held.append((qkv, ctx, inverse, in_hbm(probs)))
        w_pairs.append(weight)
    context = jnp.concatenate([h[1].reshape(2 * part_cols, frames) for h in held], 0)
    w_out_all = jnp.concatenate(w_outs, 0)
    mixed = contract(context, w_out_all, 0, 0)
    first_sum = rows_in.astype(F32) + mixed + b_out
    hidden, normed_one, inv_one = norm_forward(first_sum, gain_one, shift_one)
    low_hidden = hidden.astype(BF16)

    up_bias = [biases[r][:, 3 * part_cols :] for r in range(4)]
    acts, slopes, (total,) = ffn(low_hidden, hidden, w_ups[:2], up_bias[:2], w_downs[:2])
    more = ffn(low_hidden, total, w_ups[2:3], up_bias[2:3], w_downs[2:3])
    acts, slopes, (total,) = acts + more[0], slopes + more[1], more[2]
    grad_out = cotangent.reshape(own_clips * frames, width)
    more = ffn(low_hidden, total, w_ups[3:], up_bias[3:], w_downs[3:], grad_out, vectors)
    acts, slopes = acts + more[0], slopes + more[1]
    output, grad_two, low_two, sums_two = more[2]

    grad_w_down, grad_w_up, grad_b_up = [None] * 4, [None] * 4, [None] * 4
    grad_pre = [None] * 4
    for r in (3, 2, 1, 0):
        grad_w_down[r] = contract(acts[r], low_two, 0, 0).astype(BF16)
    far = add_low(grad_w_down[2], swap(grad_w_down[3], "mp", 1))
    d_own = sum_far(sum_near(grad_w_down[0], grad_w_down[1]), far)
    back = 0
    for r in (3, 2, 1, 0):
        grad_pre[r] = (contract(low_two, w_downs[r], 1, 1) * slopes[r].astype(F32)).astype(BF16)
        grad_b_up[r] = jnp.sum(grad_pre[r].astype(F32), 0, keepdims=True)
        grad_w_up[r] = contract(low_hidden, grad_pre[r], 0, 0).astype(BF16)
    for r in (3, 2, 1, 0):
        back = back + contract(grad_pre[r], w_ups[r], 1, 1)
    far = add_low(grad_w_up[2], swap(grad_w_up[3], "mp", 1))
    d_own, u_near = lax.optimization_barrier((d_own, sum_near(grad_w_up[0], grad_w_up[1])))
    u_own = sum_far(u_near, far)
    grad_hidden = grad_two + back
    grad_one = norm_backward(grad_hidden, normed_one, inv_one, gain_one)
    low_one = grad_one.astype(BF16)
    whole = [
        jnp.sum(rows, 0, keepdims=True)
        for rows in (
            grad_one,
            grad_hidden * normed_one,
            grad_hidden,
        )
    ]

    grad_context = contract(w_out_all, low_one, 1, 1).astype(BF16)
    grad_w_out = contract(context, low_one, 1, 0).astype(BF16).reshape(4, part_cols, width)
    grad_context = grad_context.reshape(2, 2, part_heads, HD, frames)
    units = d_own.shape[0]

    def attention_part(k, plans, events, values, collective_id):
        grads, *reduced = attend_back(
            *held[k], grad_context[k], plans, events, values, collective_id
        )
        grads = grads.reshape(6 * part_cols, frames)
        grad_w = contract(grads, rows_in, 1, 0).astype(BF16)
        pieces = []
        for r in range(2):
            piece = grad_w[3 * part_cols * r : 3 * part_cols * (r + 1)]
            pieces.append(jnp.concatenate([piece, grad_w_out[2 * k + r]], 0))
        return grads, pieces, reduced

    grads_far, pieces, (d_part,) = attention_part(
        1, ((units, True, False, D_ORDERS),), FAR_EVENTS, [d_own], 2
    )
    d_part = reduce_rest(d_part)
    far = add_low(pieces[0], swap(pieces[1], "mp", 1))
    grads_near, near, (g_down, u_part) = attention_part(
        0,
        ((units, False, True, D_ORDERS), (units, True, False, U_ORDERS)),
        NEAR_EVENTS,
        [d_part, u_own],
        3,
    )
    u_part = reduce_rest(u_part)
    own = sum_far(sum_near(near[0], near[1]), far)
    g_attn, g_up, grad_x, sums = finish(
        ((units, True, True, A_ORDERS), (units, False, True, U_ORDERS)),
        [reduce_rest(own), u_part],
        [grads_near, grads_far],
        w_pairs,
        grad_b_up + whole + [sums_two],
        grad_one,
    )
    g_attn = g_attn.astype(F32)
    for bit in bits_of("dp")[3:]:
        sums = sums + swap(sums, "dp", bit)
    grad_inputs = grad_x.reshape(inputs.shape)
    cols = part_cols
    return (
        output.reshape(inputs.shape),
        grad_inputs,
        g_attn[:cols].T,
        sums[0, :cols],
        g_attn[cols : 2 * cols].T,
        g_attn[2 * cols : 3 * cols].T,
        sums[0, 2 * cols : 3 * cols],
        g_attn[3 * cols :],
        sums[2],
        sums[3],
        sums[4],
        g_up.astype(F32),
        sums[1],
        g_down.astype(F32),
        sums[5],
        sums[6],
        sums[7],
    )


def solution(mesh):
    clips = P(("dp", "mp"), None, None)
    placed = (
        clips,
        P("dp"),
        P(None, "mp"),
        P("mp"),
        P(None, "mp"),
        P(None, "mp"),
        P("mp"),
        P("mp", None),
        P(),
        P(),
        P(),
        P(None, "mp"),
        P("mp"),
        P("mp", None),
        P(),
        P(),
        P(),
        clips,
    )
    return jax.shard_map(
        per_device,
        mesh=mesh,
        in_specs=placed,
        out_specs=(clips, clips) + placed[2:17],
        check_vma=False,
    )
```
